1024 devices in a mesh: grp: 16 (over y, x_lo), pme: 64 (over x_hi, z, core).
Axes of the slice: x: 4 (x_hi: 2, x_lo: 2; x = x_hi * 2 + x_lo), y: 8, z: 16, core: 2. Of those that a mesh axis runs over, the one named last changes fastest.
Arguments:
- charge: float32 [131072], P(('grp', 'pme')), may hold values from -4 to 4
- base: int32 [3, 131072], P(None, ('grp', 'pme')), may hold values from 0 to 255, as said below
- frac: float32 [3, 131072], P(None, ('grp', 'pme')), may hold values from 0 to 1
- counts: int32 [1024], P(('grp', 'pme')), may hold values from 16 to 128, as said below
- green: float32 [128, 256, 512], P('grp', 'pme'), may hold values from 0.05 to 0.5
Outputs:
- field: float32 [4, 131072], P(None, ('grp', 'pme'))
The draws below stay inside these ranges and needn't reach their ends.
Inputs may be any that keep to these rules, and one draw needn't show every extreme that they name: `base`: row 0 holds an atom's first mesh index along x (below 256), row 1 along y (below 256), row 2 the first of its four planes counted from the first plane of its slab (below 8). Block d's live atoms are its first counts[d] slots; other slots hold data that is ignored. Some block is full in every draw.
All inputs are finite; a program needn't handle non-finite values.
Results may differ from the reference program's by a relative error of at most 0.007.
Values may be sent and summed in bfloat16 or wider, within the bound.
No kernel may reach another device: no remote copies, remote signals or barrier semaphores. Data moves between devices by JAX's collectives and lax.ppermute only.
A program may use at most 32 MiB of HBM per device.

```python
import math
import jax
import jax.numpy as jnp
from jax import lax

NX = 256
NY = 256
NZ = 512
A_DEV = 128
KX = 128
CZ = 8
BLOCKS = 1024
ATOMS = 131072
N_PME = 64


def draw_base(key, part):
    keys = jax.random.split(jax.random.fold_in(key, 11), 3)
    along_x = jax.random.randint(keys[0], (ATOMS,), 0, NX)
    along_y = jax.random.randint(keys[1], (ATOMS,), 0, NY)
    along_z = jax.random.randint(keys[2], (ATOMS,), 0, CZ)
    return jnp.stack([along_x, along_y, along_z]).astype(jnp.int32)


def draw_counts(key, part):
    keys = jax.random.split(jax.random.fold_in(key, 23), 4)
    light = jax.random.randint(keys[0], (BLOCKS,), A_DEV // 8, A_DEV // 2 + 1)
    heavy = A_DEV - jax.random.randint(keys[1], (BLOCKS,), 0, A_DEV // 8 + 1)
    dense = jax.random.randint(keys[2], (BLOCKS,), 0, 4) == 0
    filled = jnp.where(dense, heavy, light)
    chosen = jax.random.randint(keys[3], (), 0, BLOCKS)
    filled = filled.at[chosen].set(A_DEV)
    return filled.astype(jnp.int32)


def steps_of(key, shape, shards, low, top_value):
    loudness = 1.0
    for axis_at, shards_of in shards:
        heights = jax.random.uniform(jax.random.fold_in(jax.random.fold_in(key, 6), axis_at), (shards_of,), jnp.float32, low / len(shards), top_value / len(shards))
        loudness = loudness * jnp.repeat(jnp.exp(heights), shape[axis_at] // shards_of).reshape((-1,) + (1,) * (len(shape) - 1 - axis_at))
    return loudness


def bell_draw(own_key, extent, width, limit, shards=(), held_as=jnp.bfloat16):
    array = jax.random.normal(own_key, extent, jnp.float32) * width
    if len(shards) > 0:
        array = steps_of(own_key, extent, shards, -0.22, 0.18) * array
    return jnp.clip(array, min=-limit, max=limit).astype(held_as)


def setup_inputs(seed: int = 0) -> dict:
    arg_keys = jax.random.split(jax.random.key(seed), 6)
    charge = bell_draw(arg_keys[0], (ATOMS,), 1.0, 4.0, ((0, 1024),), jnp.float32)
    base = draw_base(jax.random.fold_in(arg_keys[5], 71), 0)
    frac = jnp.clip(1.0 * jax.random.uniform(arg_keys[2], (3, ATOMS), jnp.float32) ** steps_of(arg_keys[2], (3, ATOMS), ((1, 1024),), -0.2, 0.2), 0.0, 1.0)
    counts = draw_counts(jax.random.fold_in(arg_keys[5], 71), 0)
    green = jnp.clip(jnp.exp(math.log(0.5) - 2.3025851 * jax.random.uniform(arg_keys[4], (KX, NY, NZ), jnp.float32) ** steps_of(arg_keys[4], (KX, NY, NZ), ((0, 16), (1, 64)), -0.2, 0.2)), 0.05, 0.5)
    return {"charge": charge, "base": base, "frac": frac, "counts": counts, "green": green}


TWO_PI = 2.0 * math.pi


def spline(coord):
    other = 1.0 - coord
    square = coord * coord
    cube = square * coord
    weights = jnp.stack([other * other * other / 6.0, (3.0 * cube - 6.0 * square + 4.0) / 6.0, (-3.0 * cube + 3.0 * square + 3.0 * coord + 1.0) / 6.0, cube / 6.0])
    slopes = jnp.stack([-other * other / 2.0, (3.0 * square - 4.0 * coord) / 2.0, (-3.0 * square + 2.0 * coord + 1.0) / 2.0, square / 2.0])
    return weights, slopes


def phase_parts(cell, first, count, modulus):
    waves = first + jnp.arange(count, dtype=jnp.int32)
    offsets = jnp.arange(4, dtype=jnp.int32)
    spots = (cell[None, :] + offsets[:, None]) % modulus
    turns = (spots[:, :, None] * waves[None, None, :]) % modulus
    angle = turns.astype(jnp.float32) * (TWO_PI / modulus)
    return jnp.cos(angle), jnp.sin(angle)


def combine(weights, cosine, sine):
    return jnp.sum(weights[:, :, None] * cosine, axis=0), -jnp.sum(weights[:, :, None] * sine, axis=0)


def to_bfloat(values):
    return lax.optimization_barrier(values.astype(jnp.bfloat16)).astype(jnp.float32)


def reference(charge, base, frac, counts, green):
    slots = jnp.arange(A_DEV, dtype=jnp.int32)
    live_all = (slots[None, :] < counts[:, None]).astype(jnp.float32)
    charges = charge.reshape(BLOCKS, A_DEV) * live_all
    cells = base.reshape(3, BLOCKS, A_DEV).transpose(1, 0, 2)
    coords = frac.reshape(3, BLOCKS, A_DEV).transpose(1, 0, 2)
    slab_index = (jnp.arange(BLOCKS, dtype=jnp.int32) % N_PME).astype(jnp.int32)
    offsets = jnp.arange(4, dtype=jnp.int32)

    def grid_rows(cell, slab):
        z_cells = (slab * CZ + cell[2][None, :] + offsets[:, None]) % NZ
        y_cells = (cell[1][None, :] + offsets[:, None]) % NY
        return (z_cells[:, None, :] * NY + y_cells[None, :, :]).reshape(-1)

    def deposit(grid, item):
        charge_here, cell, coord, slab = item
        x_weight, _ = spline(coord[0])
        y_weight, _ = spline(coord[1])
        z_weight, _ = spline(coord[2])
        cosine, sine = phase_parts(cell[0], 0, KX, NX)
        x_real, x_imag = combine(x_weight, cosine, sine)
        scaled = charge_here[None, :] * z_weight
        lead = jnp.stack([to_bfloat(scaled[:, :, None] * x_real[None]), to_bfloat(scaled[:, :, None] * x_imag[None])], axis=-1)
        y_low = to_bfloat(y_weight)
        update = lead[:, None] * y_low[None, :, :, None, None]
        grid = grid.at[grid_rows(cell, slab)].add(update.reshape(-1, KX, 2))
        return grid, None

    empty = jnp.zeros((NZ * NY, KX, 2), jnp.float32)
    grid, _ = lax.scan(deposit, empty, (charges, cells, coords, slab_index))
    grid = grid.reshape(NZ, NY, KX, 2)
    spectrum = (grid[..., 0] + 1j * grid[..., 1]).transpose(2, 1, 0)
    waves = jnp.fft.fftn(spectrum, axes=(1, 2))
    mesh_field = jnp.fft.ifftn(green * waves, axes=(1, 2))
    table = jnp.stack([to_bfloat(jnp.real(mesh_field)), to_bfloat(jnp.imag(mesh_field))], axis=-1)
    table = table.transpose(2, 1, 0, 3).reshape(NZ * NY, KX, 2)

    def sample(carry, item):
        charge_here, live, cell, coord, slab = item
        x_weight, x_slope = spline(coord[0])
        y_weight, y_slope = spline(coord[1])
        z_weight, z_slope = spline(coord[2])
        cosine, sine = phase_parts(cell[0], 0, KX, NX)
        x_real, x_imag = combine(x_weight, cosine, sine)
        slope_real, slope_imag = combine(x_slope, cosine, sine)
        values = table[grid_rows(cell, slab)].reshape(4, 4, A_DEV, KX, 2)
        plain_sum = jnp.sum(to_bfloat(y_weight)[None, :, :, None, None] * values, axis=1)
        slope_sum = jnp.sum(to_bfloat(y_slope)[None, :, :, None, None] * values, axis=1)
        level = jnp.sum(x_real[None] * plain_sum[..., 0] + x_imag[None] * plain_sum[..., 1], axis=-1)
        along_x = jnp.sum(slope_real[None] * plain_sum[..., 0] + slope_imag[None] * plain_sum[..., 1], axis=-1)
        along_y = jnp.sum(x_real[None] * slope_sum[..., 0] + x_imag[None] * slope_sum[..., 1], axis=-1)
        rows = jnp.stack([live * jnp.sum(z_weight * level, axis=0), charge_here * jnp.sum(z_weight * along_x, axis=0), charge_here * jnp.sum(z_weight * along_y, axis=0), charge_here * jnp.sum(z_slope * level, axis=0)])
        return carry, rows

    start = jnp.zeros((), jnp.float32)
    _, result = lax.scan(sample, start, (charges, live_all, cells, coords, slab_index))
    return result.transpose(1, 0, 2).reshape(4, BLOCKS * A_DEV)
```

```python
import functools
import math

import jax
import jax.numpy as jnp
import numpy as np
from jax import lax
from jax.experimental import pallas as pl
from jax.experimental.pallas import tpu as pltpu
from jax.sharding import PartitionSpec as P

NX = 256
NY = 256
NZ = 512
SLABS = 64
GROUPS = 16
KX = 8
KY = 4
CZ = NZ // SLABS
PLANES = CZ + 3
ATOMS = 128
LANES = 128
TWO_PI = 2.0 * math.pi

f32 = jnp.float32
bf16 = jnp.bfloat16
VMEM = pl.BlockSpec(memory_space=pltpu.VMEM)


@functools.cache
def y_table():
    wave = np.arange(NY).reshape(SLABS, 1, KY, 1)
    angle = (wave * np.arange(NY).reshape(1, 1, 1, NY) % NY) * (TWO_PI / NY)
    cosine, sine = np.cos(angle), np.sin(angle)
    real = np.stack([cosine, sine], axis=3)
    imag = np.stack([-sine, cosine], axis=3)
    return np.concatenate([real, imag], axis=1).reshape(NY * 2, NY * 2).astype(jnp.bfloat16)


@functools.cache
def slab_table():
    angle = (np.arange(SLABS)[:, None] * np.arange(128)[None, :] % SLABS) * (TWO_PI / SLABS)
    cosine, sine = np.cos(angle), np.sin(angle)
    table = np.concatenate(
        [np.concatenate([cosine, -sine], axis=1), np.concatenate([sine, cosine], axis=1)], axis=0
    )
    return table.astype(jnp.bfloat16)


@functools.cache
def plane_table():
    angle = (np.arange(16)[:, None] * np.arange(NZ)[None, :] % NZ) * (TWO_PI / NZ)
    return np.cos(angle).astype(np.float32), np.sin(angle).astype(np.float32)


def spline(u):
    other = 1.0 - u
    square = u * u
    cube = square * u
    return (
        other * other * other * (1.0 / 6.0),
        (3.0 * cube - 6.0 * square + 4.0) * (1.0 / 6.0),
        (-3.0 * cube + 3.0 * square + 3.0 * u + 1.0) * (1.0 / 6.0),
        cube * (1.0 / 6.0),
    )


def spline_slopes(u):
    other = 1.0 - u
    square = u * u
    return (
        other * other * -0.5,
        (3.0 * square - 4.0 * u) * 0.5,
        (-3.0 * square + 2.0 * u + 1.0) * 0.5,
        square * 0.5,
    )


def unit_circle(turns):
    quarter = (turns + 32) >> 6
    x = (turns - (quarter << 6)).astype(f32) * (TWO_PI / 256)
    x2 = x * x
    s = x * (1.0 + x2 * (-1.0 / 6 + x2 * (1.0 / 120 + x2 * (-1.0 / 5040 + x2 * (1.0 / 362880)))))
    c = 1.0 + x2 * (-0.5 + x2 * (1.0 / 24 + x2 * (-1.0 / 720 + x2 * (1.0 / 40320))))
    odd = (quarter & 1) == 1
    cosine = jnp.where(odd, s, c)
    sine = jnp.where(odd, c, s)
    cosine = jnp.where(((quarter + 1) & 2) == 2, -cosine, cosine)
    sine = jnp.where((quarter & 2) == 2, -sine, sine)
    return cosine, sine


def dot(a, b, dims=((1,), (0,))):
    return lax.dot_general(a, b, (dims, ((), ())), preferred_element_type=f32)


def row(values, k):
    return values[k : k + 1, :]


def x_steps(kx):
    return [unit_circle((kx * j) & (NX - 1)) for j in range(1, 4)]


def x_terms(weights, g, steps):
    even = row(weights[0], g)
    odd = 0.0
    for j in range(1, 4):
        w = row(weights[j], g)
        even = even + w * steps[j - 1][0]
        odd = odd + w * steps[j - 1][1]
    return even, odd


def turned(start, terms):
    cosine, sine = start
    even, odd = terms
    return cosine * even - sine * odd, -(sine * even + cosine * odd)


def placed(rel, weights, g):
    out = jnp.zeros(rel.shape, f32)
    for j in range(4):
        out = jnp.where(rel == j, row(weights[j], g), out)
    return out


def kernel_pack(count_hbm, charge_hbm, frac_hbm, base_hbm, out_ref, factor_ref, count_ref, charge_ref, frac_ref, base_ref, sems):
    moves = ((count_hbm, count_ref), (charge_hbm, charge_ref), (frac_hbm, frac_ref), (base_hbm, base_ref))
    copies = [pltpu.make_async_copy(a, b, sems.at[i]) for i, (a, b) in enumerate(moves)]
    for copy in copies:
        copy.start()
    for copy in copies:
        copy.wait()
    live = lax.broadcasted_iota(jnp.int32, (1, ATOMS), 1) < count_ref[0]
    loaded = jnp.where(live, charge_ref[...], 0.0)
    rows = [loaded, frac_ref[...], base_ref[...].astype(f32)]
    for g in range(GROUPS):
        out_ref[g] = jnp.concatenate(rows + [jnp.full((1, ATOMS), float(g), f32)], axis=0)
    factor_ref[...] = jnp.concatenate([jnp.where(live, 1.0, 0.0), loaded, loaded, loaded], axis=0)


def whole(values):
    return values.astype(jnp.int32)


def own_waves(atoms_ref):
    return whole(atoms_ref[0, 7:8, :]) * KX + lax.broadcasted_iota(jnp.int32, (KX, ATOMS), 0)


def kernel_spread(atoms_ref, table_ref, out_ref, y_ref, lead_ref):
    kx = own_waves(atoms_ref)
    steps = x_steps(kx)
    charge = atoms_ref[:, 0, :]
    wx, wy, wz = (spline(atoms_ref[:, 1 + d, :]) for d in range(3))
    bx, by, bz = (whole(atoms_ref[:, 4 + d, :]) for d in range(3))
    y_at = lax.broadcasted_iota(jnp.int32, (NY, ATOMS), 0)
    z_at = lax.broadcasted_iota(jnp.int32, (16, ATOMS), 0)
    wz = [charge * w for w in wz]
    blank = jnp.zeros((LANES - PLANES * KX, ATOMS), f32)
    for g in range(GROUPS):
        here = pl.ds(g * ATOMS, ATOMS)
        y_ref[:, here] = placed((y_at - row(by, g)) & (NY - 1), wy, g).astype(bf16)
        start = unit_circle((kx * row(bx, g)) & (NX - 1))
        real, imag = turned(start, x_terms(wx, g, steps))
        z = placed(z_at - row(bz, g), wz, g)
        lead = [row(z, k) * real for k in range(PLANES)] + [blank]
        lead_ref[0:LANES, here] = jnp.concatenate(lead, axis=0).astype(bf16)
        lead = [row(z, k) * imag for k in range(PLANES)] + [blank]
        lead_ref[LANES : 2 * LANES, here] = jnp.concatenate(lead, axis=0).astype(bf16)
    mesh = dot(y_ref[...], lead_ref[...], ((1,), (1,)))
    mesh = jnp.concatenate([mesh[:, :LANES], mesh[:, LANES:]], axis=0)
    waves = dot(table_ref[...], mesh.astype(bf16))
    out_ref[...] = waves.reshape(SLABS, 2 * KY, LANES).astype(bf16)


def kernel_waves(mesh_ref, green_ref, table_ref, cos_ref, sin_ref, out_ref, in_ref, hold_ref):
    in_ref[...] = mesh_ref[...].astype(f32)
    blank = jnp.zeros((LANES - PLANES * KX, 2 * LANES), f32)
    for k in range(KY):
        slabs = jnp.concatenate([in_ref[:, k, :], in_ref[:, KY + k, :]], axis=0).astype(bf16)
        part = dot(slabs, table_ref[...], ((0,), (0,)))
        real = [None] * 4
        imag = [None] * 4
        for z in range(PLANES):
            a = part[z * KX : (z + 1) * KX, :LANES]
            b = part[z * KX : (z + 1) * KX, LANES:]
            for m in range(4):
                if z == 0:
                    real[m], imag[m] = a, b
                    continue
                c = cos_ref[z : z + 1, m * LANES : (m + 1) * LANES]
                s = sin_ref[z : z + 1, m * LANES : (m + 1) * LANES]
                real[m] = real[m] + (a * c + b * s)
                imag[m] = imag[m] + (b * c - a * s)
        for m in range(4):
            factor = green_ref[:, k, m * LANES : (m + 1) * LANES] * (1.0 / (NY * NZ))
            real[m] = real[m] * factor
            imag[m] = imag[m] * factor
        rows = []
        for z in range(PLANES):
            a = b = 0.0
            for m in range(4):
                if z == 0:
                    a, b = a + real[m], b + imag[m]
                    continue
                c = cos_ref[z : z + 1, m * LANES : (m + 1) * LANES]
                s = sin_ref[z : z + 1, m * LANES : (m + 1) * LANES]
                a = a + (real[m] * c - imag[m] * s)
                b = b + (imag[m] * c + real[m] * s)
            rows.append(jnp.concatenate([a, b], axis=1))
        back = jnp.concatenate(rows + [blank], axis=0)
        cells = dot(table_ref[...], back.astype(bf16), ((1,), (1,)))
        hold_ref[:, k, :] = cells[:SLABS]
        hold_ref[:, KY + k, :] = cells[SLABS:]
    out_ref[...] = hold_ref[...].astype(bf16)


def kernel_sample(atoms_ref, mesh_ref, table_ref, out_ref, y_ref):
    kx = own_waves(atoms_ref)
    steps = x_steps(kx)
    wx, wy, wz = (spline(atoms_ref[:, 1 + d, :]) for d in range(3))
    dx, dy, dz = (spline_slopes(atoms_ref[:, 1 + d, :]) for d in range(3))
    bx, by, bz = (whole(atoms_ref[:, 4 + d, :]) for d in range(3))
    y_at = lax.broadcasted_iota(jnp.int32, (NY, ATOMS), 0)
    z_at = lax.broadcasted_iota(jnp.int32, (16, ATOMS), 0)
    waves = mesh_ref[...].reshape(2 * NY, LANES).T
    cells = dot(waves, table_ref[...]).astype(bf16)
    used = PLANES * KX
    cells = jnp.concatenate([cells[:used, :NY], cells[:used, NY:]], axis=0)
    for g in range(GROUPS):
        rel = (y_at - row(by, g)) & (NY - 1)
        y_ref[:, 0:ATOMS] = placed(rel, wy, g).astype(bf16)
        y_ref[:, ATOMS : 2 * ATOMS] = placed(rel, dy, g).astype(bf16)
        values = dot(cells, y_ref[...])
        start = unit_circle((kx * row(bx, g)) & (NX - 1))
        x_real, x_imag = turned(start, x_terms(wx, g, steps))
        s_real, s_imag = turned(start, x_terms(dx, g, steps))
        z = placed(z_at - row(bz, g), wz, g)
        dzt = placed(z_at - row(bz, g), dz, g)
        plain = [0.0, 0.0]
        along_y = [0.0, 0.0]
        along_z = [0.0, 0.0]
        for part in range(2):
            for k in range(PLANES):
                at = part * used + k * KX
                here = values[at : at + KX]
                plain[part] = plain[part] + row(z, k) * here[:, :ATOMS]
                along_y[part] = along_y[part] + row(z, k) * here[:, ATOMS:]
                along_z[part] = along_z[part] + row(dzt, k) * here[:, :ATOMS]
        terms = (
            x_real * plain[0] + x_imag * plain[1],
            s_real * plain[0] + s_imag * plain[1],
            x_real * along_y[0] + x_imag * along_y[1],
            x_real * along_z[0] + x_imag * along_z[1],
        )
        out_ref[g] = jnp.concatenate([jnp.sum(t, axis=0, keepdims=True) for t in terms], axis=0)


def kernel_total(factor_ref, terms_ref, out_ref):
    total = terms_ref[0]
    for g in range(1, GROUPS):
        total = total + terms_ref[g]
    out_ref[...] = total * factor_ref[...]


def call(kernel, shape, dtype, inputs, scratch=(), flops=0, limit=8):
    return pl.pallas_call(
        kernel,
        out_shape=jax.ShapeDtypeStruct(shape, dtype),
        in_specs=[VMEM] * inputs,
        out_specs=VMEM,
        scratch_shapes=scratch,
        name=kernel.__name__,
        compiler_params=pltpu.CompilerParams(vmem_limit_bytes=limit << 20),
        cost_estimate=pl.CostEstimate(flops=flops, bytes_accessed=1 << 20, transcendentals=0),
    )


def pack(counts, charge, frac, base):
    return pl.pallas_call(
        kernel_pack,
        out_shape=[
            jax.ShapeDtypeStruct((GROUPS, 8, ATOMS), f32),
            jax.ShapeDtypeStruct((4, ATOMS), f32),
        ],
        in_specs=[pl.BlockSpec(memory_space=pltpu.HBM)] * 4,
        out_specs=[VMEM, VMEM],
        scratch_shapes=[
            pltpu.SMEM((1,), jnp.int32),
            pltpu.VMEM((1, ATOMS), f32),
            pltpu.VMEM((3, ATOMS), f32),
            pltpu.VMEM((3, ATOMS), jnp.int32),
            pltpu.SemaphoreType.DMA((4,)),
        ],
        name="kernel_pack",
        compiler_params=pltpu.CompilerParams(vmem_limit_bytes=60 << 20),
        cost_estimate=pl.CostEstimate(flops=1 << 30, bytes_accessed=1 << 20, transcendentals=0),
    )(counts, charge, frac, base)


def spread(atoms):
    scratch = [pltpu.VMEM((NY, GROUPS * ATOMS), bf16), pltpu.VMEM((2 * LANES, GROUPS * ATOMS), bf16)]
    run = call(kernel_spread, (SLABS, 2 * KY, LANES), bf16, 2, scratch, 1 << 30)
    return run(atoms, jnp.asarray(y_table()))


def wave_product(mesh, green):
    scratch = [pltpu.VMEM((SLABS, 2 * KY, LANES), f32)] * 2
    run = call(kernel_waves, (SLABS, 2 * KY, LANES), bf16, 5, scratch, 1 << 30)
    return run(mesh, green, jnp.asarray(slab_table()), *map(jnp.asarray, plane_table()))


def sample(atoms, mesh):
    scratch = [pltpu.VMEM((NY, 2 * ATOMS), bf16)]
    run = call(kernel_sample, (GROUPS, 4, ATOMS), f32, 3, scratch, 1 << 30)
    return run(atoms, mesh, jnp.asarray(y_table()))


def total(factors, terms):
    return call(kernel_total, (4, ATOMS), f32, 2)(factors, terms)


def body(charge, base, frac, counts, green):
    charge = charge.reshape(1, ATOMS)
    swap = functools.partial(lax.all_to_all, split_axis=0, concat_axis=0, tiled=True)
    packed, factors = pack(counts, charge, frac, base)
    atoms = swap(packed, "grp")
    mesh = swap(spread(atoms), "pme")
    mesh = swap(wave_product(mesh, green), "pme")
    terms = swap(sample(atoms, mesh), "grp")
    return total(factors, terms)


def solution(mesh):
    both = ("grp", "pme")
    placed_in = (P(both), P(None, both), P(None, both), P(both), P("grp", "pme", None))
    return jax.shard_map(body, mesh=mesh, in_specs=placed_in, out_specs=P(None, both), check_vma=False)
```

```python
import functools
import math

import jax
import jax.numpy as jnp
import numpy as np
from jax import lax
from jax.experimental import pallas as pl
from jax.experimental.pallas import tpu as pltpu
from jax.sharding import PartitionSpec as P

NX = 256
NY = 256
NZ = 512
SLABS = 64
GROUPS = 16
KX = 8
KY = 4
CZ = NZ // SLABS
PLANES = CZ + 3
ATOMS = 128
LANES = 128
SPAN = 96
SENT = (SLABS, 2, KY * SPAN)
TWO_PI = 2.0 * math.pi

f32 = jnp.float32
bf16 = jnp.bfloat16
VMEM = pl.BlockSpec(memory_space=pltpu.VMEM)


@functools.cache
def y_table():
    wave = np.arange(NY).reshape(SLABS, KY).T.reshape(KY, SLABS, 1)
    angle = (wave * np.arange(NY) % NY) * (TWO_PI / NY)
    cosine, sine = np.cos(angle), np.sin(angle)
    real = np.concatenate([cosine, sine], axis=2)
    imag = np.concatenate([-sine, cosine], axis=2)
    return np.stack([real, imag], axis=2).reshape(NY * 2, NY * 2).astype(jnp.bfloat16)


@functools.cache
def slab_table():
    angle = (np.arange(SLABS)[:, None] * np.arange(128)[None, :] % SLABS) * (TWO_PI / SLABS)
    cosine, sine = np.cos(angle), np.sin(angle)
    real = np.concatenate([cosine, -sine], axis=1)
    imag = np.concatenate([sine, cosine], axis=1)
    return np.stack([real, imag], axis=1).reshape(SLABS * 2, 256).astype(jnp.bfloat16)


@functools.cache
def plane_table():
    angle = (np.arange(16)[:, None] * np.arange(NZ)[None, :] % NZ) * (TWO_PI / NZ)
    return np.cos(angle).astype(np.float32), np.sin(angle).astype(np.float32)


def spline(u):
    other = 1.0 - u
    square = u * u
    cube = square * u
    return (
        other * other * other * (1.0 / 6.0),
        (3.0 * cube - 6.0 * square + 4.0) * (1.0 / 6.0),
        (-3.0 * cube + 3.0 * square + 3.0 * u + 1.0) * (1.0 / 6.0),
        cube * (1.0 / 6.0),
    )


def spline_slopes(u):
    other = 1.0 - u
    square = u * u
    return (
        other * other * -0.5,
        (3.0 * square - 4.0 * u) * 0.5,
        (-3.0 * square + 2.0 * u + 1.0) * 0.5,
        square * 0.5,
    )


def unit_circle(turns):
    quarter = (turns + 32) >> 6
    x = (turns - (quarter << 6)).astype(f32) * (TWO_PI / 256)
    x2 = x * x
    s = x * (1.0 + x2 * (-1.0 / 6 + x2 * (1.0 / 120 + x2 * (-1.0 / 5040 + x2 * (1.0 / 362880)))))
    c = 1.0 + x2 * (-0.5 + x2 * (1.0 / 24 + x2 * (-1.0 / 720 + x2 * (1.0 / 40320))))
    odd = (quarter & 1) == 1
    cosine = jnp.where(odd, s, c)
    sine = jnp.where(odd, c, s)
    cosine = jnp.where(((quarter + 1) & 2) == 2, -cosine, cosine)
    sine = jnp.where((quarter & 2) == 2, -sine, sine)
    return cosine, sine


def dot(a, b, dims=((1,), (0,))):
    return lax.dot_general(a, b, (dims, ((), ())), preferred_element_type=f32)


def row(values, k):
    return values[k : k + 1, :]


def x_steps(kx):
    return [unit_circle((kx * j) & (NX - 1)) for j in range(1, 4)]


def x_terms(weights, g, steps):
    even = row(weights[0], g)
    odd = 0.0
    for j in range(1, 4):
        w = row(weights[j], g)
        even = even + w * steps[j - 1][0]
        odd = odd + w * steps[j - 1][1]
    return even, odd


def turned(start, terms):
    cosine, sine = start
    even, odd = terms
    return cosine * even - sine * odd, -(sine * even + cosine * odd)


def placed(rel, weights, g):
    out = jnp.zeros(rel.shape, f32)
    for j in range(4):
        out = jnp.where(rel == j, row(weights[j], g), out)
    return out


def kernel_pack(count_hbm, charge_hbm, frac_hbm, base_hbm, out_ref, factor_ref, count_ref, charge_ref, frac_ref, base_ref, sems):
    moves = ((count_hbm, count_ref), (charge_hbm, charge_ref), (frac_hbm, frac_ref), (base_hbm, base_ref))
    copies = [pltpu.make_async_copy(a, b, sems.at[i]) for i, (a, b) in enumerate(moves)]
    for copy in copies:
        copy.start()
    for copy in copies:
        copy.wait()
    live = lax.broadcasted_iota(jnp.int32, (1, ATOMS), 1) < count_ref[0]
    loaded = jnp.where(live, charge_ref[...], 0.0)
    rows = [loaded, frac_ref[...], base_ref[...].astype(f32)]
    for g in range(GROUPS):
        out_ref[g] = jnp.concatenate(rows + [jnp.full((1, ATOMS), float(g), f32)], axis=0)
    factor_ref[...] = jnp.concatenate([jnp.where(live, 1.0, 0.0), loaded, loaded, loaded], axis=0)


def whole(values):
    return values.astype(jnp.int32)


def own_waves(atoms_ref):
    return whole(atoms_ref[0, 7:8, :]) * KX + lax.broadcasted_iota(jnp.int32, (KX, ATOMS), 0)


def kernel_spread(atoms_ref, table_ref, out_ref, y_ref, lead_ref):
    kx = own_waves(atoms_ref)
    steps = x_steps(kx)
    charge = atoms_ref[:, 0, :]
    wx, wy, wz = (spline(atoms_ref[:, 1 + d, :]) for d in range(3))
    bx, by, bz = (whole(atoms_ref[:, 4 + d, :]) for d in range(3))
    y_at = lax.broadcasted_iota(jnp.int32, (NY, ATOMS), 0)
    z_at = lax.broadcasted_iota(jnp.int32, (16, ATOMS), 0)
    wz = [charge * w for w in wz]
    blank = jnp.zeros((LANES - PLANES * KX, ATOMS), f32)
    for g in range(GROUPS):
        here = pl.ds(g * ATOMS, ATOMS)
        y_ref[:, here] = placed((y_at - row(by, g)) & (NY - 1), wy, g).astype(bf16)
        start = unit_circle((kx * row(bx, g)) & (NX - 1))
        real, imag = turned(start, x_terms(wx, g, steps))
        z = placed(z_at - row(bz, g), wz, g)
        lead = [row(z, k) * real for k in range(PLANES)] + [blank]
        lead_ref[0:LANES, here] = jnp.concatenate(lead, axis=0).astype(bf16)
        lead = [row(z, k) * imag for k in range(PLANES)] + [blank]
        lead_ref[LANES : 2 * LANES, here] = jnp.concatenate(lead, axis=0).astype(bf16)
    mesh = dot(y_ref[...], lead_ref[...], ((1,), (1,)))
    mesh = jnp.concatenate([mesh[:, :LANES], mesh[:, LANES:]], axis=0)
    waves = dot(table_ref[...], mesh.astype(bf16))
    rows = 2 * SLABS
    lane = lax.broadcasted_iota(jnp.int32, (rows, LANES), 1)
    turn = [waves[k * rows : (k + 1) * rows] for k in range(KY)]
    turn = turn[:1] + [pltpu.roll(turn[k], LANES - k * (LANES - SPAN), 1) for k in range(1, KY)]
    packed = [jnp.where(lane < LANES - (k + 1) * (LANES - SPAN), turn[k], turn[k + 1]) for k in range(KY - 1)]
    out_ref[...] = jnp.concatenate(packed, axis=1).reshape(SENT).astype(bf16)


def kernel_waves(mesh_ref, green_ref, table_ref, cos_ref, sin_ref, out_ref, part_ref, back_ref):
    mesh = mesh_ref[...].reshape(2 * SLABS, KY * SPAN)
    part_ref[...] = dot(mesh, table_ref[...], ((0,), (0,)))
    blank = jnp.zeros((SPAN - PLANES * KX, 2 * LANES), f32)
    for k in range(KY):
        real = [None] * 4
        imag = [None] * 4
        for z in range(PLANES):
            at = k * SPAN + z * KX
            a = part_ref[at : at + KX, :LANES]
            b = part_ref[at : at + KX, LANES:]
            for m in range(4):
                if z == 0:
                    real[m], imag[m] = a, b
                    continue
                c = cos_ref[z : z + 1, m * LANES : (m + 1) * LANES]
                s = sin_ref[z : z + 1, m * LANES : (m + 1) * LANES]
                real[m] = real[m] + (a * c + b * s)
                imag[m] = imag[m] + (b * c - a * s)
        for m in range(4):
            factor = green_ref[:, k, m * LANES : (m + 1) * LANES] * (1.0 / (NY * NZ))
            real[m] = real[m] * factor
            imag[m] = imag[m] * factor
        rows = []
        for z in range(PLANES):
            a = b = 0.0
            for m in range(4):
                if z == 0:
                    a, b = a + real[m], b + imag[m]
                    continue
                c = cos_ref[z : z + 1, m * LANES : (m + 1) * LANES]
                s = sin_ref[z : z + 1, m * LANES : (m + 1) * LANES]
                a = a + (real[m] * c - imag[m] * s)
                b = b + (imag[m] * c + real[m] * s)
            rows.append(jnp.concatenate([a, b], axis=1))
        back_ref[k * SPAN : (k + 1) * SPAN] = jnp.concatenate(rows + [blank], axis=0).astype(bf16)
    cells = dot(table_ref[...], back_ref[...], ((1,), (1,)))
    out_ref[...] = cells.reshape(SENT).astype(bf16)


def kernel_sample(atoms_ref, mesh_ref, table_ref, out_ref, y_ref):
    kx = own_waves(atoms_ref)
    steps = x_steps(kx)
    wx, wy, wz = (spline(atoms_ref[:, 1 + d, :]) for d in range(3))
    dx, dy, dz = (spline_slopes(atoms_ref[:, 1 + d, :]) for d in range(3))
    bx, by, bz = (whole(atoms_ref[:, 4 + d, :]) for d in range(3))
    y_at = lax.broadcasted_iota(jnp.int32, (NY, ATOMS), 0)
    z_at = lax.broadcasted_iota(jnp.int32, (16, ATOMS), 0)
    waves = mesh_ref[...].reshape(2 * SLABS, KY * SPAN).T
    waves = jnp.concatenate([waves[k * SPAN : (k + 1) * SPAN] for k in range(KY)], axis=1)
    cells = dot(waves, table_ref[...]).astype(bf16)
    used = PLANES * KX
    cells = jnp.concatenate([cells[:used, :NY], cells[:used, NY:]], axis=0)
    for g in range(GROUPS):
        rel = (y_at - row(by, g)) & (NY - 1)
        y_ref[:, 0:ATOMS] = placed(rel, wy, g).astype(bf16)
        y_ref[:, ATOMS : 2 * ATOMS] = placed(rel, dy, g).astype(bf16)
        values = dot(cells, y_ref[...])
        start = unit_circle((kx * row(bx, g)) & (NX - 1))
        x_real, x_imag = turned(start, x_terms(wx, g, steps))
        s_real, s_imag = turned(start, x_terms(dx, g, steps))
        z = placed(z_at - row(bz, g), wz, g)
        dzt = placed(z_at - row(bz, g), dz, g)
        plain = [0.0, 0.0]
        along_y = [0.0, 0.0]
        along_z = [0.0, 0.0]
        for part in range(2):
            for k in range(PLANES):
                at = part * used + k * KX
                here = values[at : at + KX]
                plain[part] = plain[part] + row(z, k) * here[:, :ATOMS]
                along_y[part] = along_y[part] + row(z, k) * here[:, ATOMS:]
                along_z[part] = along_z[part] + row(dzt, k) * here[:, :ATOMS]
        terms = (
            x_real * plain[0] + x_imag * plain[1],
            s_real * plain[0] + s_imag * plain[1],
            x_real * along_y[0] + x_imag * along_y[1],
            x_real * along_z[0] + x_imag * along_z[1],
        )
        out_ref[g] = jnp.concatenate([jnp.sum(t, axis=0, keepdims=True) for t in terms], axis=0)


def kernel_total(factor_ref, terms_ref, out_ref):
    total = terms_ref[0]
    for g in range(1, GROUPS):
        total = total + terms_ref[g]
    out_ref[...] = total * factor_ref[...]


def call(kernel, shape, dtype, inputs, scratch=(), flops=0, limit=8):
    return pl.pallas_call(
        kernel,
        out_shape=jax.ShapeDtypeStruct(shape, dtype),
        in_specs=[VMEM] * inputs,
        out_specs=VMEM,
        scratch_shapes=scratch,
        name=kernel.__name__,
        compiler_params=pltpu.CompilerParams(vmem_limit_bytes=limit << 20),
        cost_estimate=pl.CostEstimate(flops=flops, bytes_accessed=1 << 20, transcendentals=0),
    )


def pack(counts, charge, frac, base):
    return pl.pallas_call(
        kernel_pack,
        out_shape=[
            jax.ShapeDtypeStruct((GROUPS, 8, ATOMS), f32),
            jax.ShapeDtypeStruct((4, ATOMS), f32),
        ],
        in_specs=[pl.BlockSpec(memory_space=pltpu.HBM)] * 4,
        out_specs=[VMEM, VMEM],
        scratch_shapes=[
            pltpu.SMEM((1,), jnp.int32),
            pltpu.VMEM((1, ATOMS), f32),
            pltpu.VMEM((3, ATOMS), f32),
            pltpu.VMEM((3, ATOMS), jnp.int32),
            pltpu.SemaphoreType.DMA((4,)),
        ],
        name="kernel_pack",
        compiler_params=pltpu.CompilerParams(vmem_limit_bytes=60 << 20),
        cost_estimate=pl.CostEstimate(flops=1 << 30, bytes_accessed=1 << 20, transcendentals=0),
    )(counts, charge, frac, base)


def spread(atoms):
    scratch = [pltpu.VMEM((NY, GROUPS * ATOMS), bf16), pltpu.VMEM((2 * LANES, GROUPS * ATOMS), bf16)]
    run = call(kernel_spread, SENT, bf16, 2, scratch, 1 << 30)
    return run(atoms, jnp.asarray(y_table()))


def wave_product(mesh, green):
    scratch = [pltpu.VMEM((KY * SPAN, 2 * LANES), f32), pltpu.VMEM((KY * SPAN, 2 * LANES), bf16)]
    run = call(kernel_waves, SENT, bf16, 5, scratch, 1 << 30)
    return run(mesh, green, jnp.asarray(slab_table()), *map(jnp.asarray, plane_table()))


def sample(atoms, mesh):
    scratch = [pltpu.VMEM((NY, 2 * ATOMS), bf16)]
    run = call(kernel_sample, (GROUPS, 4, ATOMS), f32, 3, scratch, 1 << 30)
    return run(atoms, mesh, jnp.asarray(y_table()))


def total(factors, terms):
    return call(kernel_total, (4, ATOMS), f32, 2)(factors, terms)


def body(charge, base, frac, counts, green):
    charge = charge.reshape(1, ATOMS)
    swap = functools.partial(lax.all_to_all, split_axis=0, concat_axis=0, tiled=True)
    packed, factors = pack(counts, charge, frac, base)
    atoms = swap(packed, "grp")
    mesh = swap(spread(atoms), "pme")
    mesh = swap(wave_product(mesh, green), "pme")
    terms = swap(sample(atoms, mesh), "grp")
    return total(factors, terms)


def solution(mesh):
    both = ("grp", "pme")
    placed_in = (P(both), P(None, both), P(None, both), P(both), P("grp", "pme", None))
    return jax.shard_map(body, mesh=mesh, in_specs=placed_in, out_specs=P(None, both), check_vma=False)
```

```python
import functools
import math

import jax
import jax.numpy as jnp
import numpy as np
from jax import lax
from jax.experimental import pallas as pl
from jax.experimental.pallas import tpu as pltpu
from jax.sharding import PartitionSpec as P

NX = 256
NY = 256
NZ = 512
SLABS = 64
GROUPS = 16
KX = 8
KY = 4
CZ = NZ // SLABS
PLANES = CZ + 3
ATOMS = 128
LANES = 128
SPAN = 96
SENT = (SLABS, 2, KY * SPAN)
TWO_PI = 2.0 * math.pi

f32 = jnp.float32
bf16 = jnp.bfloat16
VMEM = pl.BlockSpec(memory_space=pltpu.VMEM)


@functools.cache
def y_table():
    wave = np.arange(NY).reshape(SLABS, KY).T.reshape(KY, SLABS, 1)
    angle = (wave * np.arange(NY) % NY) * (TWO_PI / NY)
    cosine, sine = np.cos(angle), np.sin(angle)
    real = np.concatenate([cosine, sine], axis=2)
    imag = np.concatenate([-sine, cosine], axis=2)
    return np.stack([real, imag], axis=2).reshape(NY * 2, NY * 2).astype(jnp.bfloat16)


@functools.cache
def slab_table():
    angle = (np.arange(SLABS)[:, None] * np.arange(128)[None, :] % SLABS) * (TWO_PI / SLABS)
    cosine, sine = np.cos(angle), np.sin(angle)
    real = np.concatenate([cosine, -sine], axis=1)
    imag = np.concatenate([sine, cosine], axis=1)
    return np.stack([real, imag], axis=1).reshape(SLABS * 2, 256).astype(jnp.bfloat16)


@functools.cache
def plane_table():
    angle = (np.arange(16)[:, None] * np.arange(NZ)[None, :] % NZ) * (TWO_PI / NZ)
    return np.cos(angle).astype(np.float32), np.sin(angle).astype(np.float32)


def spline(u):
    other = 1.0 - u
    square = u * u
    cube = square * u
    return (
        other * other * other * (1.0 / 6.0),
        (3.0 * cube - 6.0 * square + 4.0) * (1.0 / 6.0),
        (-3.0 * cube + 3.0 * square + 3.0 * u + 1.0) * (1.0 / 6.0),
        cube * (1.0 / 6.0),
    )


def spline_slopes(u):
    other = 1.0 - u
    square = u * u
    return (
        other * other * -0.5,
        (3.0 * square - 4.0 * u) * 0.5,
        (-3.0 * square + 2.0 * u + 1.0) * 0.5,
        square * 0.5,
    )


def unit_circle(turns):
    quarter = (turns + 32) >> 6
    x = (turns - (quarter << 6)).astype(f32) * (TWO_PI / 256)
    x2 = x * x
    s = x * (1.0 + x2 * (-1.0 / 6 + x2 * (1.0 / 120 + x2 * (-1.0 / 5040 + x2 * (1.0 / 362880)))))
    c = 1.0 + x2 * (-0.5 + x2 * (1.0 / 24 + x2 * (-1.0 / 720 + x2 * (1.0 / 40320))))
    odd = (quarter & 1) == 1
    cosine = jnp.where(odd, s, c)
    sine = jnp.where(odd, c, s)
    cosine = jnp.where(((quarter + 1) & 2) == 2, -cosine, cosine)
    sine = jnp.where((quarter & 2) == 2, -sine, sine)
    return cosine, sine


def dot(a, b, dims=((1,), (0,))):
    return lax.dot_general(a, b, (dims, ((), ())), preferred_element_type=f32)


def row(values, k):
    return values[k : k + 1, :]


def x_steps(kx):
    return [unit_circle((kx * j) & (NX - 1)) for j in range(1, 4)]


def x_terms(weights, g, steps):
    even = row(weights[0], g)
    odd = 0.0
    for j in range(1, 4):
        w = row(weights[j], g)
        even = even + w * steps[j - 1][0]
        odd = odd + w * steps[j - 1][1]
    return even, odd


def turned(start, terms):
    cosine, sine = start
    even, odd = terms
    return cosine * even - sine * odd, -(sine * even + cosine * odd)


def placed(rel, weights, g):
    out = jnp.zeros(rel.shape, f32)
    for j in range(4):
        out = jnp.where(rel == j, row(weights[j], g), out)
    return out


def y_rows(at, cells, weights, g):
    out = jnp.zeros(at.shape, bf16)
    for j in range(4):
        cell = jnp.broadcast_to(row(cells[j], g), (16, ATOMS)).astype(bf16)
        weight = jnp.broadcast_to(row(weights[j], g), (16, ATOMS)).astype(bf16)
        out = jnp.where(at == tall(cell), tall(weight), out)
    return out


def tall(block):
    return jnp.concatenate([block] * (NY // 16), axis=0)


def y_cells(by):
    return [((by + j) & (NY - 1)).astype(f32) for j in range(4)]


def kernel_pack(count_ref, charge_hbm, frac_hbm, base_hbm, out_ref, factor_ref, charge_ref, frac_ref, base_ref, sems):
    moves = ((charge_hbm, charge_ref), (frac_hbm, frac_ref), (base_hbm, base_ref))
    copies = [pltpu.make_async_copy(a, b, sems.at[i]) for i, (a, b) in enumerate(moves)]
    for copy in copies:
        copy.start()
    for copy in copies:
        copy.wait()
    live = lax.broadcasted_iota(jnp.int32, (1, ATOMS), 1) < count_ref[0]
    loaded = jnp.where(live, charge_ref[...], 0.0)
    rows = [loaded, frac_ref[...], base_ref[...].astype(f32)]
    for g in range(GROUPS):
        out_ref[g] = jnp.concatenate(rows + [jnp.full((1, ATOMS), float(g), f32)], axis=0)
    factor_ref[...] = jnp.concatenate([jnp.where(live, 1.0, 0.0), loaded, loaded, loaded], axis=0)


def whole(values):
    return values.astype(jnp.int32)


def own_waves(atoms_ref):
    return whole(atoms_ref[0, 7:8, :]) * KX + lax.broadcasted_iota(jnp.int32, (KX, ATOMS), 0)


def kernel_spread(atoms_ref, table_ref, out_ref, y_ref, lead_ref):
    kx = own_waves(atoms_ref)
    steps = x_steps(kx)
    charge = atoms_ref[:, 0, :]
    wx, wy, wz = (spline(atoms_ref[:, 1 + d, :]) for d in range(3))
    bx, by, bz = (whole(atoms_ref[:, 4 + d, :]) for d in range(3))
    y_at = lax.broadcasted_iota(jnp.int32, (NY, ATOMS), 0).astype(f32).astype(bf16)
    ys = y_cells(by)
    z_at = lax.broadcasted_iota(jnp.int32, (16, ATOMS), 0)
    wz = [charge * w for w in wz]
    blank = jnp.zeros((LANES - PLANES * KX, ATOMS), f32)
    for g in range(GROUPS):
        here = pl.ds(g * ATOMS, ATOMS)
        y_ref[:, here] = y_rows(y_at, ys, wy, g)
        start = unit_circle((kx * row(bx, g)) & (NX - 1))
        real, imag = turned(start, x_terms(wx, g, steps))
        z = placed(z_at - row(bz, g), wz, g)
        lead = [row(z, k) * real for k in range(PLANES)] + [blank]
        lead_ref[0:LANES, here] = jnp.concatenate(lead, axis=0).astype(bf16)
        lead = [row(z, k) * imag for k in range(PLANES)] + [blank]
        lead_ref[LANES : 2 * LANES, here] = jnp.concatenate(lead, axis=0).astype(bf16)
    mesh = dot(y_ref[...], lead_ref[...], ((1,), (1,)))
    mesh = jnp.concatenate([mesh[:, :LANES], mesh[:, LANES:]], axis=0)
    waves = dot(table_ref[...], mesh.astype(bf16))
    rows = 2 * SLABS
    lane = lax.broadcasted_iota(jnp.int32, (rows, LANES), 1)
    turn = [waves[k * rows : (k + 1) * rows] for k in range(KY)]
    turn = turn[:1] + [pltpu.roll(turn[k], LANES - k * (LANES - SPAN), 1) for k in range(1, KY)]
    packed = [jnp.where(lane < LANES - (k + 1) * (LANES - SPAN), turn[k], turn[k + 1]) for k in range(KY - 1)]
    out_ref[...] = jnp.concatenate(packed, axis=1).astype(bf16).reshape(SENT)


def kernel_waves(mesh_ref, green_ref, table_ref, cos_ref, sin_ref, out_ref, part_ref, back_ref):
    mesh = mesh_ref[...].reshape(2 * SLABS, KY * SPAN)
    part_ref[...] = dot(mesh, table_ref[...], ((0,), (0,)))
    blank = jnp.zeros((SPAN - PLANES * KX, 2 * LANES), f32)
    for k in range(KY):
        real = [None] * 4
        imag = [None] * 4
        for z in range(PLANES):
            at = k * SPAN + z * KX
            a = part_ref[at : at + KX, :LANES]
            b = part_ref[at : at + KX, LANES:]
            for m in range(4):
                if z == 0:
                    real[m], imag[m] = a, b
                    continue
                c = cos_ref[z : z + 1, m * LANES : (m + 1) * LANES]
                s = sin_ref[z : z + 1, m * LANES : (m + 1) * LANES]
                real[m] = real[m] + (a * c + b * s)
                imag[m] = imag[m] + (b * c - a * s)
        for m in range(4):
            factor = green_ref[:, k, m * LANES : (m + 1) * LANES] * (1.0 / (NY * NZ))
            real[m] = real[m] * factor
            imag[m] = imag[m] * factor
        rows = []
        for z in range(PLANES):
            a = b = 0.0
            for m in range(4):
                if z == 0:
                    a, b = a + real[m], b + imag[m]
                    continue
                c = cos_ref[z : z + 1, m * LANES : (m + 1) * LANES]
                s = sin_ref[z : z + 1, m * LANES : (m + 1) * LANES]
                a = a + (real[m] * c - imag[m] * s)
                b = b + (imag[m] * c + real[m] * s)
            rows.append(jnp.concatenate([a, b], axis=1))
        back_ref[k * SPAN : (k + 1) * SPAN] = jnp.concatenate(rows + [blank], axis=0).astype(bf16)
    cells = dot(table_ref[...], back_ref[...], ((1,), (1,)))
    out_ref[...] = cells.astype(bf16).reshape(SENT)


def kernel_sample(atoms_ref, mesh_ref, table_ref, out_ref, y_ref):
    kx = own_waves(atoms_ref)
    steps = x_steps(kx)
    wx, wy, wz = (spline(atoms_ref[:, 1 + d, :]) for d in range(3))
    dx, dy, dz = (spline_slopes(atoms_ref[:, 1 + d, :]) for d in range(3))
    bx, by, bz = (whole(atoms_ref[:, 4 + d, :]) for d in range(3))
    y_at = lax.broadcasted_iota(jnp.int32, (NY, ATOMS), 0).astype(f32).astype(bf16)
    ys = y_cells(by)
    z_at = lax.broadcasted_iota(jnp.int32, (16, ATOMS), 0)
    waves = mesh_ref[...].reshape(2 * SLABS, KY * SPAN).T
    waves = jnp.concatenate([waves[k * SPAN : (k + 1) * SPAN] for k in range(KY)], axis=1)
    cells = dot(waves, table_ref[...]).astype(bf16)
    used = PLANES * KX
    cells = jnp.concatenate([cells[:used, :NY], cells[:used, NY:]], axis=0)
    for g in range(GROUPS):
        y_ref[:, 0:ATOMS] = y_rows(y_at, ys, wy, g)
        y_ref[:, ATOMS : 2 * ATOMS] = y_rows(y_at, ys, dy, g)
        values = dot(cells, y_ref[...])
        start = unit_circle((kx * row(bx, g)) & (NX - 1))
        x_real, x_imag = turned(start, x_terms(wx, g, steps))
        s_real, s_imag = turned(start, x_terms(dx, g, steps))
        z = placed(z_at - row(bz, g), wz, g)
        dzt = placed(z_at - row(bz, g), dz, g)
        plain = [0.0, 0.0]
        along_y = [0.0, 0.0]
        along_z = [0.0, 0.0]
        for part in range(2):
            for k in range(PLANES):
                at = part * used + k * KX
                here = values[at : at + KX]
                plain[part] = plain[part] + row(z, k) * here[:, :ATOMS]
                along_y[part] = along_y[part] + row(z, k) * here[:, ATOMS:]
                along_z[part] = along_z[part] + row(dzt, k) * here[:, :ATOMS]
        terms = (
            x_real * plain[0] + x_imag * plain[1],
            s_real * plain[0] + s_imag * plain[1],
            x_real * along_y[0] + x_imag * along_y[1],
            x_real * along_z[0] + x_imag * along_z[1],
        )
        out_ref[g] = jnp.concatenate([jnp.sum(t, axis=0, keepdims=True) for t in terms], axis=0)


def kernel_total(factor_ref, terms_ref, out_ref):
    total = terms_ref[0]
    for g in range(1, GROUPS):
        total = total + terms_ref[g]
    out_ref[...] = total * factor_ref[...]


def call(kernel, shape, dtype, inputs, scratch=(), flops=0, limit=8):
    return pl.pallas_call(
        kernel,
        out_shape=jax.ShapeDtypeStruct(shape, dtype),
        in_specs=[VMEM] * inputs,
        out_specs=VMEM,
        scratch_shapes=scratch,
        name=kernel.__name__,
        compiler_params=pltpu.CompilerParams(vmem_limit_bytes=limit << 20),
        cost_estimate=pl.CostEstimate(flops=flops, bytes_accessed=1 << 20, transcendentals=0),
    )


def pack(counts, charge, frac, base):
    return pl.pallas_call(
        kernel_pack,
        out_shape=[
            jax.ShapeDtypeStruct((GROUPS, 8, ATOMS), f32),
            jax.ShapeDtypeStruct((4, ATOMS), f32),
        ],
        in_specs=[pl.BlockSpec(memory_space=pltpu.SMEM)] + [pl.BlockSpec(memory_space=pltpu.HBM)] * 3,
        out_specs=[VMEM, VMEM],
        scratch_shapes=[
            pltpu.VMEM((1, ATOMS), f32),
            pltpu.VMEM((3, ATOMS), f32),
            pltpu.VMEM((3, ATOMS), jnp.int32),
            pltpu.SemaphoreType.DMA((3,)),
        ],
        name="kernel_pack",
        compiler_params=pltpu.CompilerParams(vmem_limit_bytes=4 << 20),
        cost_estimate=pl.CostEstimate(flops=1 << 30, bytes_accessed=1 << 20, transcendentals=0),
    )(counts, *(pltpu.with_memory_space_constraint(a, pltpu.HBM) for a in (charge, frac, base)))


def spread(atoms):
    scratch = [pltpu.VMEM((NY, GROUPS * ATOMS), bf16), pltpu.VMEM((2 * LANES, GROUPS * ATOMS), bf16)]
    run = call(kernel_spread, SENT, bf16, 2, scratch, 1 << 30)
    return run(atoms, jnp.asarray(y_table()))


def wave_product(mesh, green):
    scratch = [pltpu.VMEM((KY * SPAN, 2 * LANES), f32), pltpu.VMEM((KY * SPAN, 2 * LANES), bf16)]
    run = call(kernel_waves, SENT, bf16, 5, scratch, 1 << 30)
    return run(mesh, green, jnp.asarray(slab_table()), *map(jnp.asarray, plane_table()))


def sample(atoms, mesh):
    scratch = [pltpu.VMEM((NY, 2 * ATOMS), bf16)]
    run = call(kernel_sample, (GROUPS, 4, ATOMS), f32, 3, scratch, 1 << 30)
    return run(atoms, mesh, jnp.asarray(y_table()))


def total(factors, terms):
    return call(kernel_total, (4, ATOMS), f32, 2)(factors, terms)


def body(charge, base, frac, counts, green):
    charge = charge.reshape(1, ATOMS)
    swap = functools.partial(lax.all_to_all, split_axis=0, concat_axis=0, tiled=True)
    packed, factors = pack(counts, charge, frac, base)
    atoms = swap(packed, "grp")
    mesh = swap(spread(atoms), "pme")
    mesh = swap(wave_product(mesh, green), "pme")
    terms = swap(sample(atoms, mesh), "grp")
    return total(factors, terms)


def solution(mesh):
    both = ("grp", "pme")
    placed_in = (P(both), P(None, both), P(None, both), P(both), P("grp", "pme", None))
    return jax.shard_map(body, mesh=mesh, in_specs=placed_in, out_specs=P(None, both), check_vma=False)
```

```python
import functools
import math

import jax
import jax.numpy as jnp
import numpy as np
from jax import lax
from jax.experimental import pallas as pl
from jax.experimental.pallas import tpu as pltpu
from jax.sharding import PartitionSpec as P

NX = 256
NY = 256
NZ = 512
SLABS = 64
GROUPS = 16
KX = 8
KY = 4
CZ = NZ // SLABS
PLANES = CZ + 3
ATOMS = 128
LANES = 128
SPAN = 96
SENT = (SLABS, 2, KY * SPAN)
TWO_PI = 2.0 * math.pi

f32 = jnp.float32
bf16 = jnp.bfloat16
VMEM = pl.BlockSpec(memory_space=pltpu.VMEM)


@functools.cache
def y_table():
    wave = np.arange(NY).reshape(SLABS, KY).T.reshape(KY, SLABS, 1)
    angle = (wave * np.arange(NY) % NY) * (TWO_PI / NY)
    cosine, sine = np.cos(angle), np.sin(angle)
    real = np.concatenate([cosine, sine], axis=2)
    imag = np.concatenate([-sine, cosine], axis=2)
    return np.stack([real, imag], axis=2).reshape(NY * 2, NY * 2).astype(jnp.bfloat16)


@functools.cache
def slab_table():
    angle = (np.arange(SLABS)[:, None] * np.arange(128)[None, :] % SLABS) * (TWO_PI / SLABS)
    cosine, sine = np.cos(angle), np.sin(angle)
    real = np.concatenate([cosine, -sine], axis=1)
    imag = np.concatenate([sine, cosine], axis=1)
    return np.stack([real, imag], axis=1).reshape(SLABS * 2, 256).astype(jnp.bfloat16)


@functools.cache
def plane_table():
    angle = (np.arange(16)[:, None] * np.arange(NZ)[None, :] % NZ) * (TWO_PI / NZ)
    return np.cos(angle).astype(np.float32), np.sin(angle).astype(np.float32)


def spline(u):
    other = 1.0 - u
    square = u * u
    cube = square * u
    return (
        other * other * other * (1.0 / 6.0),
        (3.0 * cube - 6.0 * square + 4.0) * (1.0 / 6.0),
        (-3.0 * cube + 3.0 * square + 3.0 * u + 1.0) * (1.0 / 6.0),
        cube * (1.0 / 6.0),
    )


def spline_slopes(u):
    other = 1.0 - u
    square = u * u
    return (
        other * other * -0.5,
        (3.0 * square - 4.0 * u) * 0.5,
        (-3.0 * square + 2.0 * u + 1.0) * 0.5,
        square * 0.5,
    )


def unit_circle(turns):
    quarter = (turns + 32) >> 6
    x = (turns - (quarter << 6)).astype(f32) * (TWO_PI / 256)
    x2 = x * x
    s = x * (1.0 + x2 * (-1.0 / 6 + x2 * (1.0 / 120 + x2 * (-1.0 / 5040 + x2 * (1.0 / 362880)))))
    c = 1.0 + x2 * (-0.5 + x2 * (1.0 / 24 + x2 * (-1.0 / 720 + x2 * (1.0 / 40320))))
    odd = (quarter & 1) == 1
    cosine = jnp.where(odd, s, c)
    sine = jnp.where(odd, c, s)
    cosine = jnp.where(((quarter + 1) & 2) == 2, -cosine, cosine)
    sine = jnp.where((quarter & 2) == 2, -sine, sine)
    return cosine, sine


def dot(a, b, dims=((1,), (0,))):
    return lax.dot_general(a, b, (dims, ((), ())), preferred_element_type=f32)


def row(values, k):
    return values[k : k + 1, :]


def x_steps(kx):
    return [unit_circle((kx * j) & (NX - 1)) for j in range(1, 4)]


def x_terms(weights, g, steps):
    even = row(weights[0], g)
    odd = 0.0
    for j in range(1, 4):
        w = row(weights[j], g)
        even = even + w * steps[j - 1][0]
        odd = odd + w * steps[j - 1][1]
    return even, odd


def turned(start, terms):
    cosine, sine = start
    even, odd = terms
    return cosine * even - sine * odd, -(sine * even + cosine * odd)


def placed(rel, weights, g):
    out = jnp.zeros(rel.shape, f32)
    for j in range(4):
        out = jnp.where(rel == j, row(weights[j], g), out)
    return out


def y_rows(at, cells, weights, g):
    out = jnp.zeros(at.shape, bf16)
    for j in range(4):
        cell = jnp.broadcast_to(row(cells[j], g), (16, ATOMS)).astype(bf16)
        weight = jnp.broadcast_to(row(weights[j], g), (16, ATOMS)).astype(bf16)
        out = jnp.where(at == tall(cell), tall(weight), out)
    return out


def tall(block):
    return jnp.concatenate([block] * (NY // 16), axis=0)


def y_cells(by):
    return [((by + j) & (NY - 1)).astype(f32) for j in range(4)]


def kernel_pack(count_ref, charge_hbm, frac_hbm, base_hbm, out_ref, factor_ref, charge_ref, frac_ref, base_ref, sems):
    moves = ((charge_hbm, charge_ref), (frac_hbm, frac_ref), (base_hbm, base_ref))
    copies = [pltpu.make_async_copy(a, b, sems.at[i]) for i, (a, b) in enumerate(moves)]
    for copy in copies:
        copy.start()
    for copy in copies:
        copy.wait()
    live = lax.broadcasted_iota(jnp.int32, (1, ATOMS), 1) < count_ref[0]
    loaded = jnp.where(live, charge_ref[...], 0.0)
    rows = [loaded, frac_ref[...], base_ref[...].astype(f32)]
    for g in range(GROUPS):
        out_ref[g] = jnp.concatenate(rows + [jnp.full((1, ATOMS), float(g), f32)], axis=0)
    factor_ref[...] = jnp.concatenate([jnp.where(live, 1.0, 0.0), loaded, loaded, loaded], axis=0)


def whole(values):
    return values.astype(jnp.int32)


def own_waves(atoms_ref):
    return whole(atoms_ref[0, 7:8, :]) * KX + lax.broadcasted_iota(jnp.int32, (KX, ATOMS), 0)


def kernel_spread(atoms_ref, table_ref, out_ref, y_ref, x_ref, lead_ref):
    kx = own_waves(atoms_ref)
    steps = x_steps(kx)
    charge = atoms_ref[:, 0, :]
    wx, wy, wz = (spline(atoms_ref[:, 1 + d, :]) for d in range(3))
    bx, by, bz = (whole(atoms_ref[:, 4 + d, :]) for d in range(3))
    y_at = lax.broadcasted_iota(jnp.int32, (NY, ATOMS), 0).astype(f32).astype(bf16)
    ys = y_cells(by)
    z_at = lax.broadcasted_iota(jnp.int32, (16, ATOMS), 0)
    wz = [charge * w for w in wz]
    blank = jnp.zeros((LANES - PLANES * KX, ATOMS), f32)
    for g in range(GROUPS):
        here = pl.ds(g * ATOMS, ATOMS)
        y_ref[:, here] = y_rows(y_at, ys, wy, g)
        start = unit_circle((kx * row(bx, g)) & (NX - 1))
        real, imag = turned(start, x_terms(wx, g, steps))
        for k, values in enumerate((real, imag) + start):
            x_ref[k, :, here] = values
        z = placed(z_at - row(bz, g), wz, g)
        lead = [row(z, k) * real for k in range(PLANES)] + [blank]
        lead_ref[0:LANES, here] = jnp.concatenate(lead, axis=0).astype(bf16)
        lead = [row(z, k) * imag for k in range(PLANES)] + [blank]
        lead_ref[LANES : 2 * LANES, here] = jnp.concatenate(lead, axis=0).astype(bf16)
    mesh = dot(y_ref[...], lead_ref[...], ((1,), (1,)))
    mesh = jnp.concatenate([mesh[:, :LANES], mesh[:, LANES:]], axis=0)
    waves = dot(table_ref[...], mesh.astype(bf16))
    rows = 2 * SLABS
    lane = lax.broadcasted_iota(jnp.int32, (rows, LANES), 1)
    turn = [waves[k * rows : (k + 1) * rows] for k in range(KY)]
    turn = turn[:1] + [pltpu.roll(turn[k], LANES - k * (LANES - SPAN), 1) for k in range(1, KY)]
    packed = [jnp.where(lane < LANES - (k + 1) * (LANES - SPAN), turn[k], turn[k + 1]) for k in range(KY - 1)]
    out_ref[...] = jnp.concatenate(packed, axis=1).astype(bf16).reshape(SENT)


def kernel_waves(mesh_ref, green_ref, table_ref, cos_ref, sin_ref, out_ref, part_ref, back_ref):
    mesh = mesh_ref[...].reshape(2 * SLABS, KY * SPAN)
    part_ref[...] = dot(mesh, table_ref[...], ((0,), (0,)))
    blank = jnp.zeros((SPAN - PLANES * KX, 2 * LANES), f32)
    for k in range(KY):
        real = [None] * 4
        imag = [None] * 4
        for z in range(PLANES):
            at = k * SPAN + z * KX
            a = part_ref[at : at + KX, :LANES]
            b = part_ref[at : at + KX, LANES:]
            for m in range(4):
                if z == 0:
                    real[m], imag[m] = a, b
                    continue
                c = cos_ref[z : z + 1, m * LANES : (m + 1) * LANES]
                s = sin_ref[z : z + 1, m * LANES : (m + 1) * LANES]
                real[m] = real[m] + (a * c + b * s)
                imag[m] = imag[m] + (b * c - a * s)
        for m in range(4):
            factor = green_ref[:, k, m * LANES : (m + 1) * LANES] * (1.0 / (NY * NZ))
            real[m] = real[m] * factor
            imag[m] = imag[m] * factor
        rows = []
        for z in range(PLANES):
            a = b = 0.0
            for m in range(4):
                if z == 0:
                    a, b = a + real[m], b + imag[m]
                    continue
                c = cos_ref[z : z + 1, m * LANES : (m + 1) * LANES]
                s = sin_ref[z : z + 1, m * LANES : (m + 1) * LANES]
                a = a + (real[m] * c - imag[m] * s)
                b = b + (imag[m] * c + real[m] * s)
            rows.append(jnp.concatenate([a, b], axis=1))
        back_ref[k * SPAN : (k + 1) * SPAN] = jnp.concatenate(rows + [blank], axis=0).astype(bf16)
    cells = dot(table_ref[...], back_ref[...], ((1,), (1,)))
    out_ref[...] = cells.astype(bf16).reshape(SENT)


def kernel_sample(atoms_ref, mesh_ref, table_ref, y_ref, x_ref, out_ref, slope_ref):
    kx = own_waves(atoms_ref)
    steps = x_steps(kx)
    wz = spline(atoms_ref[:, 3, :])
    dx, dy, dz = (spline_slopes(atoms_ref[:, 1 + d, :]) for d in range(3))
    by, bz = (whole(atoms_ref[:, 4 + d, :]) for d in range(1, 3))
    y_at = lax.broadcasted_iota(jnp.int32, (NY, ATOMS), 0).astype(f32).astype(bf16)
    ys = y_cells(by)
    z_at = lax.broadcasted_iota(jnp.int32, (16, ATOMS), 0)
    waves = mesh_ref[...].reshape(2 * SLABS, KY * SPAN).T
    waves = jnp.concatenate([waves[k * SPAN : (k + 1) * SPAN] for k in range(KY)], axis=1)
    cells = dot(waves, table_ref[...]).astype(bf16)
    used = PLANES * KX
    cells = jnp.concatenate([cells[:used, :NY], cells[:used, NY:]], axis=0)

    def sample_block(g, level, slope):
        x_real, x_imag, *start = (x_ref[k, :, pl.ds(g * ATOMS, ATOMS)] for k in range(4))
        s_real, s_imag = turned(start, x_terms(dx, g, steps))
        z = placed(z_at - row(bz, g), wz, g)
        dzt = placed(z_at - row(bz, g), dz, g)
        plain = [0.0, 0.0]
        along_y = [0.0, 0.0]
        along_z = [0.0, 0.0]
        for part in range(2):
            for k in range(PLANES):
                at = part * used + k * KX
                here = level[at : at + KX]
                there = slope[at : at + KX]
                plain[part] = plain[part] + row(z, k) * here
                along_y[part] = along_y[part] + row(z, k) * there
                along_z[part] = along_z[part] + row(dzt, k) * here
        terms = (
            x_real * plain[0] + x_imag * plain[1],
            s_real * plain[0] + s_imag * plain[1],
            x_real * along_y[0] + x_imag * along_y[1],
            x_real * along_z[0] + x_imag * along_z[1],
        )
        out_ref[g] = jnp.concatenate([jnp.sum(t, axis=0, keepdims=True) for t in terms], axis=0)

    for g in range(GROUPS):
        here = pl.ds(g * ATOMS, ATOMS)
        slope_ref[:, here] = y_rows(y_at, ys, dy, g)
        if g % 2 == 0:
            continue
        both = pl.ds((g - 1) * ATOMS, 2 * ATOMS)
        level = dot(cells, y_ref[:, both])
        slope = dot(cells, slope_ref[:, both])
        for h in range(2):
            at = slice(h * ATOMS, (h + 1) * ATOMS)
            sample_block(g - 1 + h, level[:, at], slope[:, at])


def kernel_total(factor_ref, terms_ref, out_ref):
    total = terms_ref[0]
    for g in range(1, GROUPS):
        total = total + terms_ref[g]
    out_ref[...] = total * factor_ref[...]


def call(kernel, shape, dtype, inputs, scratch=(), flops=0, limit=8):
    return pl.pallas_call(
        kernel,
        out_shape=jax.ShapeDtypeStruct(shape, dtype),
        in_specs=[VMEM] * inputs,
        out_specs=VMEM,
        scratch_shapes=scratch,
        name=kernel.__name__,
        compiler_params=pltpu.CompilerParams(vmem_limit_bytes=limit << 20),
        cost_estimate=pl.CostEstimate(flops=flops, bytes_accessed=1 << 20, transcendentals=0),
    )


def pack(counts, charge, frac, base):
    return pl.pallas_call(
        kernel_pack,
        out_shape=[
            jax.ShapeDtypeStruct((GROUPS, 8, ATOMS), f32),
            jax.ShapeDtypeStruct((4, ATOMS), f32),
        ],
        in_specs=[pl.BlockSpec(memory_space=pltpu.SMEM)] + [pl.BlockSpec(memory_space=pltpu.HBM)] * 3,
        out_specs=[VMEM, VMEM],
        scratch_shapes=[
            pltpu.VMEM((1, ATOMS), f32),
            pltpu.VMEM((3, ATOMS), f32),
            pltpu.VMEM((3, ATOMS), jnp.int32),
            pltpu.SemaphoreType.DMA((3,)),
        ],
        name="kernel_pack",
        compiler_params=pltpu.CompilerParams(vmem_limit_bytes=4 << 20),
        cost_estimate=pl.CostEstimate(flops=1 << 30, bytes_accessed=1 << 20, transcendentals=0),
    )(counts, *(pltpu.with_memory_space_constraint(a, pltpu.HBM) for a in (charge, frac, base)))


def spread(atoms):
    return pl.pallas_call(
        kernel_spread,
        out_shape=[
            jax.ShapeDtypeStruct(SENT, bf16),
            jax.ShapeDtypeStruct((NY, GROUPS * ATOMS), bf16),
            jax.ShapeDtypeStruct((4, KX, GROUPS * ATOMS), f32),
        ],
        in_specs=[VMEM] * 2,
        out_specs=[VMEM] * 3,
        scratch_shapes=[pltpu.VMEM((2 * LANES, GROUPS * ATOMS), bf16)],
        name="kernel_spread",
        compiler_params=pltpu.CompilerParams(vmem_limit_bytes=8 << 20),
        cost_estimate=pl.CostEstimate(flops=1 << 30, bytes_accessed=1 << 20, transcendentals=0),
    )(atoms, jnp.asarray(y_table()))


def wave_product(mesh, green):
    scratch = [pltpu.VMEM((KY * SPAN, 2 * LANES), f32), pltpu.VMEM((KY * SPAN, 2 * LANES), bf16)]
    run = call(kernel_waves, SENT, bf16, 5, scratch, 1 << 30)
    return run(mesh, green, jnp.asarray(slab_table()), *map(jnp.asarray, plane_table()))


def sample(atoms, mesh, y_weights, x_sums):
    scratch = [pltpu.VMEM((NY, GROUPS * ATOMS), bf16)]
    run = call(kernel_sample, (GROUPS, 4, ATOMS), f32, 5, scratch, 1 << 30)
    return run(atoms, mesh, jnp.asarray(y_table()), y_weights, x_sums)


def total(factors, terms):
    return call(kernel_total, (4, ATOMS), f32, 2)(factors, terms)


def body(charge, base, frac, counts, green):
    charge = charge.reshape(1, ATOMS)
    swap = functools.partial(lax.all_to_all, split_axis=0, concat_axis=0, tiled=True)
    packed, factors = pack(counts, charge, frac, base)
    atoms = swap(packed, "grp")
    mesh, y_weights, x_sums = spread(atoms)
    mesh = swap(mesh, "pme")
    mesh = swap(wave_product(mesh, green), "pme")
    terms = swap(sample(atoms, mesh, y_weights, x_sums), "grp")
    return total(factors, terms)


def solution(mesh):
    both = ("grp", "pme")
    placed_in = (P(both), P(None, both), P(None, both), P(both), P("grp", "pme", None))
    return jax.shard_map(body, mesh=mesh, in_specs=placed_in, out_specs=P(None, both), check_vma=False)
```

```python
import functools
import math

import jax
import jax.numpy as jnp
import numpy as np
from jax import lax
from jax.experimental import pallas as pl
from jax.experimental.pallas import tpu as pltpu
from jax.sharding import PartitionSpec as P

NX = 256
NY = 256
NZ = 512
SLABS = 64
GROUPS = 16
KX = 8
KY = 4
CZ = NZ // SLABS
PLANES = CZ + 3
ATOMS = 128
LANES = 128
SPAN = 96
SENT = (SLABS, 2, KY * SPAN)
TWO_PI = 2.0 * math.pi

f32 = jnp.float32
bf16 = jnp.bfloat16
VMEM = pl.BlockSpec(memory_space=pltpu.VMEM)


@functools.cache
def y_table():
    wave = np.arange(NY).reshape(SLABS, KY).T.reshape(KY, SLABS, 1)
    angle = (wave * np.arange(NY) % NY) * (TWO_PI / NY)
    cosine, sine = np.cos(angle), np.sin(angle)
    real = np.concatenate([cosine, sine], axis=2)
    imag = np.concatenate([-sine, cosine], axis=2)
    return np.stack([real, imag], axis=2).reshape(NY * 2, NY * 2).astype(jnp.bfloat16)


@functools.cache
def slab_table():
    angle = (np.arange(SLABS)[:, None] * np.arange(128)[None, :] % SLABS) * (TWO_PI / SLABS)
    cosine, sine = np.cos(angle), np.sin(angle)
    real = np.concatenate([cosine, -sine], axis=1)
    imag = np.concatenate([sine, cosine], axis=1)
    return np.stack([real, imag], axis=1).reshape(SLABS * 2, 256).astype(jnp.bfloat16)


@functools.cache
def plane_table():
    angle = (np.arange(16)[:, None] * np.arange(NZ)[None, :] % NZ) * (TWO_PI / NZ)
    return np.cos(angle).astype(np.float32), np.sin(angle).astype(np.float32)


def spline(u):
    other = 1.0 - u
    square = u * u
    cube = square * u
    return (
        other * other * other * (1.0 / 6.0),
        (3.0 * cube - 6.0 * square + 4.0) * (1.0 / 6.0),
        (-3.0 * cube + 3.0 * square + 3.0 * u + 1.0) * (1.0 / 6.0),
        cube * (1.0 / 6.0),
    )


def spline_slopes(u):
    other = 1.0 - u
    square = u * u
    return (
        other * other * -0.5,
        (3.0 * square - 4.0 * u) * 0.5,
        (-3.0 * square + 2.0 * u + 1.0) * 0.5,
        square * 0.5,
    )


def unit_circle(turns):
    quarter = (turns + 32) >> 6
    x = (turns - (quarter << 6)).astype(f32) * (TWO_PI / 256)
    x2 = x * x
    s = x * (1.0 + x2 * (-1.0 / 6 + x2 * (1.0 / 120 + x2 * (-1.0 / 5040 + x2 * (1.0 / 362880)))))
    c = 1.0 + x2 * (-0.5 + x2 * (1.0 / 24 + x2 * (-1.0 / 720 + x2 * (1.0 / 40320))))
    odd = (quarter & 1) == 1
    cosine = jnp.where(odd, s, c)
    sine = jnp.where(odd, c, s)
    cosine = jnp.where(((quarter + 1) & 2) == 2, -cosine, cosine)
    sine = jnp.where((quarter & 2) == 2, -sine, sine)
    return cosine, sine


def dot(a, b, dims=((1,), (0,))):
    return lax.dot_general(a, b, (dims, ((), ())), preferred_element_type=f32)


def row(values, k):
    return values[k : k + 1, :]


def x_steps(kx):
    return [unit_circle((kx * j) & (NX - 1)) for j in range(1, 4)]


def x_terms(weights, g, steps):
    even = row(weights[0], g)
    odd = 0.0
    for j in range(1, 4):
        w = row(weights[j], g)
        even = even + w * steps[j - 1][0]
        odd = odd + w * steps[j - 1][1]
    return even, odd


def turned(start, terms):
    cosine, sine = start
    even, odd = terms
    return cosine * even - sine * odd, -(sine * even + cosine * odd)


def placed(rel, weights, g):
    out = jnp.zeros(rel.shape, f32)
    for j in range(4):
        out = jnp.where(rel == j, row(weights[j], g), out)
    return out


def y_rows(spots, weights, g):
    block, local, *weights = (
        jnp.broadcast_to(row(v, g), (16, ATOMS)).astype(bf16) for v in (*spots, *weights)
    )
    nothing = jnp.zeros((16, ATOMS), bf16)
    rel = lax.broadcasted_iota(jnp.int32, (16, ATOMS), 0).astype(f32).astype(bf16) - local
    low = high = nothing
    for j in range(4):
        low = jnp.where(rel == j, weights[j], low)
        high = jnp.where(rel == j - 16, weights[j], high)
    own = [block == b for b in range(16)]
    return jnp.concatenate(
        [jnp.where(own[b], low, jnp.where(own[b - 1], high, nothing)) for b in range(16)], axis=0
    )


def y_spots(by):
    return (by >> 4).astype(f32), (by & 15).astype(f32)


def kernel_pack(count_ref, charge_hbm, frac_hbm, base_hbm, out_ref, factor_ref, charge_ref, frac_ref, base_ref, sems):
    moves = ((charge_hbm, charge_ref), (frac_hbm, frac_ref), (base_hbm, base_ref))
    copies = [pltpu.make_async_copy(a, b, sems.at[i]) for i, (a, b) in enumerate(moves)]
    for copy in copies:
        copy.start()
    for copy in copies:
        copy.wait()
    live = lax.broadcasted_iota(jnp.int32, (1, ATOMS), 1) < count_ref[0]
    loaded = jnp.where(live, charge_ref[...], 0.0)
    rows = [loaded, frac_ref[...], base_ref[...].astype(f32)]
    for g in range(GROUPS):
        out_ref[g] = jnp.concatenate(rows + [jnp.full((1, ATOMS), float(g), f32)], axis=0)
    factor_ref[...] = jnp.concatenate([jnp.where(live, 1.0, 0.0), loaded, loaded, loaded], axis=0)


def whole(values):
    return values.astype(jnp.int32)


def own_waves(atoms_ref):
    return whole(atoms_ref[0, 7:8, :]) * KX + lax.broadcasted_iota(jnp.int32, (KX, ATOMS), 0)


def kernel_spread(atoms_ref, table_ref, out_ref, y_ref, x_ref, lead_ref):
    kx = own_waves(atoms_ref)
    steps = x_steps(kx)
    charge = atoms_ref[:, 0, :]
    wx, wy, wz = (spline(atoms_ref[:, 1 + d, :]) for d in range(3))
    bx, by, bz = (whole(atoms_ref[:, 4 + d, :]) for d in range(3))
    ys = y_spots(by)
    z_at = lax.broadcasted_iota(jnp.int32, (16, ATOMS), 0)
    wz = [charge * w for w in wz]
    blank = jnp.zeros((LANES - PLANES * KX, ATOMS), f32)
    for g in range(GROUPS):
        here = pl.ds(g * ATOMS, ATOMS)
        y_ref[:, here] = y_rows(ys, wy, g)
        start = unit_circle((kx * row(bx, g)) & (NX - 1))
        real, imag = turned(start, x_terms(wx, g, steps))
        for k, values in enumerate((real, imag) + start):
            x_ref[k, :, here] = values
        z = placed(z_at - row(bz, g), wz, g)
        lead = [row(z, k) * real for k in range(PLANES)] + [blank]
        lead_ref[0:LANES, here] = jnp.concatenate(lead, axis=0).astype(bf16)
        lead = [row(z, k) * imag for k in range(PLANES)] + [blank]
        lead_ref[LANES : 2 * LANES, here] = jnp.concatenate(lead, axis=0).astype(bf16)
    mesh = dot(y_ref[...], lead_ref[...], ((1,), (1,)))
    mesh = jnp.concatenate([mesh[:, :LANES], mesh[:, LANES:]], axis=0)
    waves = dot(table_ref[...], mesh.astype(bf16))
    rows = 2 * SLABS
    lane = lax.broadcasted_iota(jnp.int32, (rows, LANES), 1)
    turn = [waves[k * rows : (k + 1) * rows] for k in range(KY)]
    turn = turn[:1] + [pltpu.roll(turn[k], LANES - k * (LANES - SPAN), 1) for k in range(1, KY)]
    packed = [jnp.where(lane < LANES - (k + 1) * (LANES - SPAN), turn[k], turn[k + 1]) for k in range(KY - 1)]
    out_ref[...] = jnp.concatenate(packed, axis=1).astype(bf16).reshape(SENT)


def kernel_waves(mesh_ref, green_ref, table_ref, cos_ref, sin_ref, out_ref, part_ref, back_ref):
    mesh = mesh_ref[...].reshape(2 * SLABS, KY * SPAN)
    part_ref[...] = dot(mesh, table_ref[...], ((0,), (0,)))
    blank = jnp.zeros((SPAN - PLANES * KX, 2 * LANES), f32)
    for k in range(KY):
        real = [None] * 4
        imag = [None] * 4
        for z in range(PLANES):
            at = k * SPAN + z * KX
            a = part_ref[at : at + KX, :LANES]
            b = part_ref[at : at + KX, LANES:]
            for m in range(4):
                if z == 0:
                    real[m], imag[m] = a, b
                    continue
                c = cos_ref[z : z + 1, m * LANES : (m + 1) * LANES]
                s = sin_ref[z : z + 1, m * LANES : (m + 1) * LANES]
                real[m] = real[m] + (a * c + b * s)
                imag[m] = imag[m] + (b * c - a * s)
        for m in range(4):
            factor = green_ref[:, k, m * LANES : (m + 1) * LANES] * (1.0 / (NY * NZ))
            real[m] = real[m] * factor
            imag[m] = imag[m] * factor
        rows = []
        for z in range(PLANES):
            a = b = 0.0
            for m in range(4):
                if z == 0:
                    a, b = a + real[m], b + imag[m]
                    continue
                c = cos_ref[z : z + 1, m * LANES : (m + 1) * LANES]
                s = sin_ref[z : z + 1, m * LANES : (m + 1) * LANES]
                a = a + (real[m] * c - imag[m] * s)
                b = b + (imag[m] * c + real[m] * s)
            rows.append(jnp.concatenate([a, b], axis=1))
        back_ref[k * SPAN : (k + 1) * SPAN] = jnp.concatenate(rows + [blank], axis=0).astype(bf16)
    cells = dot(table_ref[...], back_ref[...], ((1,), (1,)))
    out_ref[...] = cells.astype(bf16).reshape(SENT)


def kernel_sample(atoms_ref, mesh_ref, table_ref, y_ref, x_ref, out_ref, slope_ref):
    kx = own_waves(atoms_ref)
    steps = x_steps(kx)
    wz = spline(atoms_ref[:, 3, :])
    dx, dy, dz = (spline_slopes(atoms_ref[:, 1 + d, :]) for d in range(3))
    by, bz = (whole(atoms_ref[:, 4 + d, :]) for d in range(1, 3))
    ys = y_spots(by)
    z_at = lax.broadcasted_iota(jnp.int32, (16, ATOMS), 0)
    waves = mesh_ref[...].reshape(2 * SLABS, KY * SPAN).T
    waves = jnp.concatenate([waves[k * SPAN : (k + 1) * SPAN] for k in range(KY)], axis=1)
    cells = dot(waves, table_ref[...]).astype(bf16)
    used = PLANES * KX
    cells = jnp.concatenate([cells[:used, :NY], cells[:used, NY:]], axis=0)

    def sample_block(g, level, slope):
        x_real, x_imag, *start = (x_ref[k, :, pl.ds(g * ATOMS, ATOMS)] for k in range(4))
        s_real, s_imag = turned(start, x_terms(dx, g, steps))
        z = placed(z_at - row(bz, g), wz, g)
        dzt = placed(z_at - row(bz, g), dz, g)
        plain = [0.0, 0.0]
        along_y = [0.0, 0.0]
        along_z = [0.0, 0.0]
        for part in range(2):
            for k in range(PLANES):
                at = part * used + k * KX
                here = level[at : at + KX]
                there = slope[at : at + KX]
                plain[part] = plain[part] + row(z, k) * here
                along_y[part] = along_y[part] + row(z, k) * there
                along_z[part] = along_z[part] + row(dzt, k) * here
        terms = (
            x_real * plain[0] + x_imag * plain[1],
            s_real * plain[0] + s_imag * plain[1],
            x_real * along_y[0] + x_imag * along_y[1],
            x_real * along_z[0] + x_imag * along_z[1],
        )
        out_ref[g] = jnp.concatenate([jnp.sum(t, axis=0, keepdims=True) for t in terms], axis=0)

    for g in range(GROUPS):
        here = pl.ds(g * ATOMS, ATOMS)
        slope_ref[:, here] = y_rows(ys, dy, g)
        if g % 2 == 0:
            continue
        both = pl.ds((g - 1) * ATOMS, 2 * ATOMS)
        level = dot(cells, y_ref[:, both])
        slope = dot(cells, slope_ref[:, both])
        for h in range(2):
            at = slice(h * ATOMS, (h + 1) * ATOMS)
            sample_block(g - 1 + h, level[:, at], slope[:, at])


def kernel_total(factor_ref, terms_ref, out_ref):
    total = terms_ref[0]
    for g in range(1, GROUPS):
        total = total + terms_ref[g]
    out_ref[...] = total * factor_ref[...]


def call(kernel, shape, dtype, inputs, scratch=(), flops=0, limit=8):
    return pl.pallas_call(
        kernel,
        out_shape=jax.ShapeDtypeStruct(shape, dtype),
        in_specs=[VMEM] * inputs,
        out_specs=VMEM,
        scratch_shapes=scratch,
        name=kernel.__name__,
        compiler_params=pltpu.CompilerParams(vmem_limit_bytes=limit << 20),
        cost_estimate=pl.CostEstimate(flops=flops, bytes_accessed=1 << 20, transcendentals=0),
    )


def pack(counts, charge, frac, base):
    return pl.pallas_call(
        kernel_pack,
        out_shape=[
            jax.ShapeDtypeStruct((GROUPS, 8, ATOMS), f32),
            jax.ShapeDtypeStruct((4, ATOMS), f32),
        ],
        in_specs=[pl.BlockSpec(memory_space=pltpu.SMEM)] + [pl.BlockSpec(memory_space=pltpu.HBM)] * 3,
        out_specs=[VMEM, VMEM],
        scratch_shapes=[
            pltpu.VMEM((1, ATOMS), f32),
            pltpu.VMEM((3, ATOMS), f32),
            pltpu.VMEM((3, ATOMS), jnp.int32),
            pltpu.SemaphoreType.DMA((3,)),
        ],
        name="kernel_pack",
        compiler_params=pltpu.CompilerParams(vmem_limit_bytes=4 << 20),
        cost_estimate=pl.CostEstimate(flops=1 << 30, bytes_accessed=1 << 20, transcendentals=0),
    )(counts, *(pltpu.with_memory_space_constraint(a, pltpu.HBM) for a in (charge, frac, base)))


def spread(atoms):
    return pl.pallas_call(
        kernel_spread,
        out_shape=[
            jax.ShapeDtypeStruct(SENT, bf16),
            jax.ShapeDtypeStruct((NY, GROUPS * ATOMS), bf16),
            jax.ShapeDtypeStruct((4, KX, GROUPS * ATOMS), f32),
        ],
        in_specs=[VMEM] * 2,
        out_specs=[VMEM] * 3,
        scratch_shapes=[pltpu.VMEM((2 * LANES, GROUPS * ATOMS), bf16)],
        name="kernel_spread",
        compiler_params=pltpu.CompilerParams(vmem_limit_bytes=8 << 20),
        cost_estimate=pl.CostEstimate(flops=1 << 30, bytes_accessed=1 << 20, transcendentals=0),
    )(atoms, jnp.asarray(y_table()))


def wave_product(mesh, green):
    scratch = [pltpu.VMEM((KY * SPAN, 2 * LANES), f32), pltpu.VMEM((KY * SPAN, 2 * LANES), bf16)]
    run = call(kernel_waves, SENT, bf16, 5, scratch, 1 << 30)
    return run(mesh, green, jnp.asarray(slab_table()), *map(jnp.asarray, plane_table()))


def sample(atoms, mesh, y_weights, x_sums):
    scratch = [pltpu.VMEM((NY, GROUPS * ATOMS), bf16)]
    run = call(kernel_sample, (GROUPS, 4, ATOMS), f32, 5, scratch, 1 << 30)
    return run(atoms, mesh, jnp.asarray(y_table()), y_weights, x_sums)


def total(factors, terms):
    return call(kernel_total, (4, ATOMS), f32, 2)(factors, terms)


def body(charge, base, frac, counts, green):
    charge = charge.reshape(1, ATOMS)
    swap = functools.partial(lax.all_to_all, split_axis=0, concat_axis=0, tiled=True)
    packed, factors = pack(counts, charge, frac, base)
    atoms = swap(packed, "grp")
    mesh, y_weights, x_sums = spread(atoms)
    mesh = swap(mesh, "pme")
    mesh = swap(wave_product(mesh, green), "pme")
    terms = swap(sample(atoms, mesh, y_weights, x_sums), "grp")
    return total(factors, terms)


def solution(mesh):
    both = ("grp", "pme")
    placed_in = (P(both), P(None, both), P(None, both), P(both), P("grp", "pme", None))
    return jax.shard_map(body, mesh=mesh, in_specs=placed_in, out_specs=P(None, both), check_vma=False)
```

```python
import functools
import math

import jax
import jax.numpy as jnp
import numpy as np
from jax import lax
from jax.experimental import pallas as pl
from jax.experimental.pallas import tpu as pltpu
from jax.sharding import PartitionSpec as P

NX = 256
NY = 256
NZ = 512
SLABS = 64
GROUPS = 16
KX = 8
KY = 4
CZ = NZ // SLABS
PLANES = CZ + 3
ATOMS = 128
LANES = 128
SPAN = 96
SENT = (SLABS, 2, KY * SPAN)
TWO_PI = 2.0 * math.pi

f32 = jnp.float32
bf16 = jnp.bfloat16
VMEM = pl.BlockSpec(memory_space=pltpu.VMEM)


@functools.cache
def y_table():
    wave = np.arange(NY).reshape(SLABS, KY).T.reshape(KY, SLABS, 1)
    angle = (wave * np.arange(NY) % NY) * (TWO_PI / NY)
    cosine, sine = np.cos(angle), np.sin(angle)
    real = np.concatenate([cosine, sine], axis=2)
    imag = np.concatenate([-sine, cosine], axis=2)
    return np.stack([real, imag], axis=2).reshape(NY * 2, NY * 2).astype(jnp.bfloat16)


@functools.cache
def slab_table():
    angle = (np.arange(SLABS)[:, None] * np.arange(128)[None, :] % SLABS) * (TWO_PI / SLABS)
    cosine, sine = np.cos(angle), np.sin(angle)
    real = np.concatenate([cosine, -sine], axis=1)
    imag = np.concatenate([sine, cosine], axis=1)
    return np.stack([real, imag], axis=1).reshape(SLABS * 2, 256).astype(jnp.bfloat16)


@functools.cache
def plane_table():
    angle = (np.arange(16)[:, None] * np.arange(NZ)[None, :] % NZ) * (TWO_PI / NZ)
    return np.cos(angle).astype(np.float32), np.sin(angle).astype(np.float32)


def spline(u):
    other = 1.0 - u
    square = u * u
    cube = square * u
    return (
        other * other * other * (1.0 / 6.0),
        (3.0 * cube - 6.0 * square + 4.0) * (1.0 / 6.0),
        (-3.0 * cube + 3.0 * square + 3.0 * u + 1.0) * (1.0 / 6.0),
        cube * (1.0 / 6.0),
    )


def spline_slopes(u):
    other = 1.0 - u
    square = u * u
    return (
        other * other * -0.5,
        (3.0 * square - 4.0 * u) * 0.5,
        (-3.0 * square + 2.0 * u + 1.0) * 0.5,
        square * 0.5,
    )


def unit_circle(turns):
    quarter = (turns + 32) >> 6
    x = (turns - (quarter << 6)).astype(f32) * (TWO_PI / 256)
    x2 = x * x
    s = x * (1.0 + x2 * (-1.0 / 6 + x2 * (1.0 / 120 + x2 * (-1.0 / 5040 + x2 * (1.0 / 362880)))))
    c = 1.0 + x2 * (-0.5 + x2 * (1.0 / 24 + x2 * (-1.0 / 720 + x2 * (1.0 / 40320))))
    odd = (quarter & 1) == 1
    cosine = jnp.where(odd, s, c)
    sine = jnp.where(odd, c, s)
    cosine = jnp.where(((quarter + 1) & 2) == 2, -cosine, cosine)
    sine = jnp.where((quarter & 2) == 2, -sine, sine)
    return cosine, sine


def dot(a, b, dims=((1,), (0,))):
    return lax.dot_general(a, b, (dims, ((), ())), preferred_element_type=f32)


def row(values, k):
    return values[k : k + 1, :]


def x_steps(kx):
    return [unit_circle((kx * j) & (NX - 1)) for j in range(1, 4)]


def x_terms(weights, g, steps):
    even = row(weights[0], g)
    odd = 0.0
    for j in range(1, 4):
        w = row(weights[j], g)
        even = even + w * steps[j - 1][0]
        odd = odd + w * steps[j - 1][1]
    return even, odd


def turned(start, terms):
    cosine, sine = start
    even, odd = terms
    return cosine * even - sine * odd, -(sine * even + cosine * odd)


def placed(rel, weights, g):
    out = jnp.zeros(rel.shape, f32)
    for j in range(4):
        out = jnp.where(rel == j, row(weights[j], g), out)
    return out


def y_rows(spots, weights, g):
    block, local, *weights = (
        jnp.broadcast_to(row(v, g), (16, ATOMS)).astype(bf16) for v in (*spots, *weights)
    )
    nothing = jnp.zeros((16, ATOMS), bf16)
    rel = lax.broadcasted_iota(jnp.int32, (16, ATOMS), 0).astype(f32).astype(bf16) - local
    low = high = nothing
    for j in range(4):
        low = jnp.where(rel == j, weights[j], low)
        high = jnp.where(rel == j - 16, weights[j], high)
    own = [block == b for b in range(16)]
    return jnp.concatenate(
        [jnp.where(own[b], low, jnp.where(own[b - 1], high, nothing)) for b in range(16)], axis=0
    )


def y_spots(by):
    return (by >> 4).astype(f32), (by & 15).astype(f32)


def kernel_pack(count_ref, charge_hbm, frac_hbm, base_hbm, out_ref, factor_ref, charge_ref, frac_ref, base_ref, sems):
    moves = ((charge_hbm, charge_ref), (frac_hbm, frac_ref), (base_hbm, base_ref))
    copies = [pltpu.make_async_copy(a, b, sems.at[i]) for i, (a, b) in enumerate(moves)]
    for copy in copies:
        copy.start()
    for copy in copies:
        copy.wait()
    live = lax.broadcasted_iota(jnp.int32, (1, ATOMS), 1) < count_ref[0]
    loaded = jnp.where(live, charge_ref[...], 0.0)
    rows = [loaded, frac_ref[...], base_ref[...].astype(f32)]
    for g in range(GROUPS):
        out_ref[g] = jnp.concatenate(rows + [jnp.full((1, ATOMS), float(g), f32)], axis=0)
    factor_ref[...] = jnp.concatenate([jnp.where(live, 1.0, 0.0), loaded, loaded, loaded], axis=0)


def whole(values):
    return values.astype(jnp.int32)


def own_waves(atoms_ref):
    return whole(atoms_ref[7, 0:1, :]) * KX + lax.broadcasted_iota(jnp.int32, (KX, ATOMS), 0)


def kernel_spread(sent_ref, table_ref, out_ref, y_ref, x_ref, atoms_ref, lead_ref):
    for k in range(8):
        atoms_ref[k] = sent_ref[:, k, :]
    kx = own_waves(atoms_ref)
    steps = x_steps(kx)
    charge = atoms_ref[0]
    wx, wy, wz = (spline(atoms_ref[1 + d]) for d in range(3))
    bx, by, bz = (whole(atoms_ref[4 + d]) for d in range(3))
    ys = y_spots(by)
    z_at = lax.broadcasted_iota(jnp.int32, (16, ATOMS), 0)
    wz = [charge * w for w in wz]
    blank = jnp.zeros((LANES - PLANES * KX, ATOMS), f32)
    for g in range(GROUPS):
        here = pl.ds(g * ATOMS, ATOMS)
        y_ref[:, here] = y_rows(ys, wy, g)
        start = unit_circle((kx * row(bx, g)) & (NX - 1))
        real, imag = turned(start, x_terms(wx, g, steps))
        for k, values in enumerate((real, imag) + start):
            x_ref[k, :, here] = values
        z = placed(z_at - row(bz, g), wz, g)
        lead = [row(z, k) * real for k in range(PLANES)] + [blank]
        lead_ref[0:LANES, here] = jnp.concatenate(lead, axis=0).astype(bf16)
        lead = [row(z, k) * imag for k in range(PLANES)] + [blank]
        lead_ref[LANES : 2 * LANES, here] = jnp.concatenate(lead, axis=0).astype(bf16)
    mesh = dot(y_ref[...], lead_ref[...], ((1,), (1,)))
    mesh = jnp.concatenate([mesh[:, :LANES], mesh[:, LANES:]], axis=0)
    waves = dot(table_ref[...], mesh.astype(bf16))
    rows = 2 * SLABS
    lane = lax.broadcasted_iota(jnp.int32, (rows, LANES), 1)
    turn = [waves[k * rows : (k + 1) * rows] for k in range(KY)]
    turn = turn[:1] + [pltpu.roll(turn[k], LANES - k * (LANES - SPAN), 1) for k in range(1, KY)]
    packed = [jnp.where(lane < LANES - (k + 1) * (LANES - SPAN), turn[k], turn[k + 1]) for k in range(KY - 1)]
    out_ref[...] = jnp.concatenate(packed, axis=1).astype(bf16).reshape(SENT)


def kernel_waves(mesh_ref, green_ref, table_ref, cos_ref, sin_ref, out_ref, part_ref, back_ref):
    mesh = mesh_ref[...].reshape(2 * SLABS, KY * SPAN)
    part_ref[...] = dot(mesh, table_ref[...], ((0,), (0,)))
    blank = jnp.zeros((SPAN - PLANES * KX, 2 * LANES), f32)
    for k in range(KY):
        real = [None] * 4
        imag = [None] * 4
        for z in range(PLANES):
            at = k * SPAN + z * KX
            a = part_ref[at : at + KX, :LANES]
            b = part_ref[at : at + KX, LANES:]
            for m in range(4):
                if z == 0:
                    real[m], imag[m] = a, b
                    continue
                c = cos_ref[z : z + 1, m * LANES : (m + 1) * LANES]
                s = sin_ref[z : z + 1, m * LANES : (m + 1) * LANES]
                real[m] = real[m] + (a * c + b * s)
                imag[m] = imag[m] + (b * c - a * s)
        for m in range(4):
            factor = green_ref[:, k, m * LANES : (m + 1) * LANES] * (1.0 / (NY * NZ))
            real[m] = real[m] * factor
            imag[m] = imag[m] * factor
        rows = []
        for z in range(PLANES):
            a = b = 0.0
            for m in range(4):
                if z == 0:
                    a, b = a + real[m], b + imag[m]
                    continue
                c = cos_ref[z : z + 1, m * LANES : (m + 1) * LANES]
                s = sin_ref[z : z + 1, m * LANES : (m + 1) * LANES]
                a = a + (real[m] * c - imag[m] * s)
                b = b + (imag[m] * c + real[m] * s)
            rows.append(jnp.concatenate([a, b], axis=1))
        back_ref[k * SPAN : (k + 1) * SPAN] = jnp.concatenate(rows + [blank], axis=0).astype(bf16)
    cells = dot(table_ref[...], back_ref[...], ((1,), (1,)))
    out_ref[...] = cells.astype(bf16).reshape(SENT)


def kernel_sample(atoms_ref, mesh_ref, table_ref, y_ref, x_ref, out_ref, slope_ref):
    kx = own_waves(atoms_ref)
    steps = x_steps(kx)
    wz = spline(atoms_ref[3])
    dx, dy, dz = (spline_slopes(atoms_ref[1 + d]) for d in range(3))
    by, bz = (whole(atoms_ref[4 + d]) for d in range(1, 3))
    ys = y_spots(by)
    z_at = lax.broadcasted_iota(jnp.int32, (16, ATOMS), 0)
    waves = mesh_ref[...].reshape(2 * SLABS, KY * SPAN).T
    waves = jnp.concatenate([waves[k * SPAN : (k + 1) * SPAN] for k in range(KY)], axis=1)
    cells = dot(waves, table_ref[...]).astype(bf16)
    used = PLANES * KX
    cells = jnp.concatenate([cells[:used, :NY], cells[:used, NY:]], axis=0)

    def sample_block(g, level, slope):
        x_real, x_imag, *start = (x_ref[k, :, pl.ds(g * ATOMS, ATOMS)] for k in range(4))
        s_real, s_imag = turned(start, x_terms(dx, g, steps))
        z = placed(z_at - row(bz, g), wz, g)
        dzt = placed(z_at - row(bz, g), dz, g)
        plain = [0.0, 0.0]
        along_y = [0.0, 0.0]
        along_z = [0.0, 0.0]
        for part in range(2):
            for k in range(PLANES):
                at = part * used + k * KX
                here = level[at : at + KX]
                there = slope[at : at + KX]
                plain[part] = plain[part] + row(z, k) * here
                along_y[part] = along_y[part] + row(z, k) * there
                along_z[part] = along_z[part] + row(dzt, k) * here
        terms = (
            x_real * plain[0] + x_imag * plain[1],
            s_real * plain[0] + s_imag * plain[1],
            x_real * along_y[0] + x_imag * along_y[1],
            x_real * along_z[0] + x_imag * along_z[1],
        )
        out_ref[g] = jnp.concatenate([jnp.sum(t, axis=0, keepdims=True) for t in terms], axis=0)

    for g in range(GROUPS):
        here = pl.ds(g * ATOMS, ATOMS)
        slope_ref[:, here] = y_rows(ys, dy, g)
        if g % 2 == 0:
            continue
        both = pl.ds((g - 1) * ATOMS, 2 * ATOMS)
        level = dot(cells, y_ref[:, both])
        slope = dot(cells, slope_ref[:, both])
        for h in range(2):
            at = slice(h * ATOMS, (h + 1) * ATOMS)
            sample_block(g - 1 + h, level[:, at], slope[:, at])


def kernel_total(factor_ref, terms_ref, out_ref):
    total = terms_ref[0]
    for g in range(1, GROUPS):
        total = total + terms_ref[g]
    out_ref[...] = total * factor_ref[...]


def call(kernel, shape, dtype, inputs, scratch=(), flops=0, limit=8):
    return pl.pallas_call(
        kernel,
        out_shape=jax.ShapeDtypeStruct(shape, dtype),
        in_specs=[VMEM] * inputs,
        out_specs=VMEM,
        scratch_shapes=scratch,
        name=kernel.__name__,
        compiler_params=pltpu.CompilerParams(vmem_limit_bytes=limit << 20),
        cost_estimate=pl.CostEstimate(flops=flops, bytes_accessed=1 << 20, transcendentals=0),
    )


def pack(counts, charge, frac, base):
    return pl.pallas_call(
        kernel_pack,
        out_shape=[
            jax.ShapeDtypeStruct((GROUPS, 8, ATOMS), f32),
            jax.ShapeDtypeStruct((4, ATOMS), f32),
        ],
        in_specs=[pl.BlockSpec(memory_space=pltpu.SMEM)] + [pl.BlockSpec(memory_space=pltpu.HBM)] * 3,
        out_specs=[VMEM, VMEM],
        scratch_shapes=[
            pltpu.VMEM((1, ATOMS), f32),
            pltpu.VMEM((3, ATOMS), f32),
            pltpu.VMEM((3, ATOMS), jnp.int32),
            pltpu.SemaphoreType.DMA((3,)),
        ],
        name="kernel_pack",
        compiler_params=pltpu.CompilerParams(vmem_limit_bytes=4 << 20),
        cost_estimate=pl.CostEstimate(flops=1 << 30, bytes_accessed=1 << 20, transcendentals=0),
    )(counts, *(pltpu.with_memory_space_constraint(a, pltpu.HBM) for a in (charge, frac, base)))


def spread(atoms):
    return pl.pallas_call(
        kernel_spread,
        out_shape=[
            jax.ShapeDtypeStruct(SENT, bf16),
            jax.ShapeDtypeStruct((NY, GROUPS * ATOMS), bf16),
            jax.ShapeDtypeStruct((4, KX, GROUPS * ATOMS), f32),
            jax.ShapeDtypeStruct((8, GROUPS, ATOMS), f32),
        ],
        in_specs=[VMEM] * 2,
        out_specs=[VMEM] * 4,
        scratch_shapes=[pltpu.VMEM((2 * LANES, GROUPS * ATOMS), bf16)],
        name="kernel_spread",
        compiler_params=pltpu.CompilerParams(vmem_limit_bytes=8 << 20),
        cost_estimate=pl.CostEstimate(flops=1 << 30, bytes_accessed=1 << 20, transcendentals=0),
    )(atoms, jnp.asarray(y_table()))


def wave_product(mesh, green):
    scratch = [pltpu.VMEM((KY * SPAN, 2 * LANES), f32), pltpu.VMEM((KY * SPAN, 2 * LANES), bf16)]
    run = call(kernel_waves, SENT, bf16, 5, scratch, 1 << 30)
    return run(mesh, green, jnp.asarray(slab_table()), *map(jnp.asarray, plane_table()))


def sample(atoms, mesh, y_weights, x_sums):
    scratch = [pltpu.VMEM((NY, GROUPS * ATOMS), bf16)]
    run = call(kernel_sample, (GROUPS, 4, ATOMS), f32, 5, scratch, 1 << 30)
    return run(atoms, mesh, jnp.asarray(y_table()), y_weights, x_sums)


def total(factors, terms):
    return call(kernel_total, (4, ATOMS), f32, 2)(factors, terms)


def body(charge, base, frac, counts, green):
    charge = charge.reshape(1, ATOMS)
    swap = functools.partial(lax.all_to_all, split_axis=0, concat_axis=0, tiled=True)
    packed, factors = pack(counts, charge, frac, base)
    atoms = swap(packed, "grp")
    mesh, y_weights, x_sums, atoms = spread(atoms)
    mesh = swap(mesh, "pme")
    mesh = swap(wave_product(mesh, green), "pme")
    terms = swap(sample(atoms, mesh, y_weights, x_sums), "grp")
    return total(factors, terms)


def solution(mesh):
    both = ("grp", "pme")
    placed_in = (P(both), P(None, both), P(None, both), P(both), P("grp", "pme", None))
    return jax.shard_map(body, mesh=mesh, in_specs=placed_in, out_specs=P(None, both), check_vma=False)
```

```python
import functools
import math

import jax
import jax.numpy as jnp
import numpy as np
from jax import lax
from jax.experimental import pallas as pl
from jax.experimental.pallas import tpu as pltpu
from jax.sharding import PartitionSpec as P

NX = 256
NY = 256
NZ = 512
SLABS = 64
GROUPS = 16
KX = 8
KY = 4
CZ = NZ // SLABS
PLANES = CZ + 3
ATOMS = 128
LANES = 128
SPAN = 96
SENT = (SLABS, 2, KY * SPAN)
TWO_PI = 2.0 * math.pi

f32 = jnp.float32
bf16 = jnp.bfloat16
VMEM = pl.BlockSpec(memory_space=pltpu.VMEM)


@functools.cache
def y_table():
    wave = np.arange(NY).reshape(SLABS, KY).T.reshape(KY, SLABS, 1)
    angle = (wave * np.arange(NY) % NY) * (TWO_PI / NY)
    cosine, sine = np.cos(angle), np.sin(angle)
    real = np.concatenate([cosine, sine], axis=2)
    imag = np.concatenate([-sine, cosine], axis=2)
    return np.stack([real, imag], axis=2).reshape(NY * 2, NY * 2).astype(jnp.bfloat16)


@functools.cache
def slab_table():
    angle = (np.arange(SLABS)[:, None] * np.arange(128)[None, :] % SLABS) * (TWO_PI / SLABS)
    cosine, sine = np.cos(angle), np.sin(angle)
    real = np.concatenate([cosine, -sine], axis=1)
    imag = np.concatenate([sine, cosine], axis=1)
    return np.stack([real, imag], axis=1).reshape(SLABS * 2, 256).astype(jnp.bfloat16)


@functools.cache
def plane_table():
    angle = (np.arange(16)[:, None] * np.arange(NZ)[None, :] % NZ) * (TWO_PI / NZ)
    return np.cos(angle).astype(np.float32), np.sin(angle).astype(np.float32)


def spline(u):
    other = 1.0 - u
    square = u * u
    cube = square * u
    return (
        other * other * other * (1.0 / 6.0),
        (3.0 * cube - 6.0 * square + 4.0) * (1.0 / 6.0),
        (-3.0 * cube + 3.0 * square + 3.0 * u + 1.0) * (1.0 / 6.0),
        cube * (1.0 / 6.0),
    )


def spline_slopes(u):
    other = 1.0 - u
    square = u * u
    return (
        other * other * -0.5,
        (3.0 * square - 4.0 * u) * 0.5,
        (-3.0 * square + 2.0 * u + 1.0) * 0.5,
        square * 0.5,
    )


def unit_circle(turns):
    quarter = (turns + 32) >> 6
    x = (turns - (quarter << 6)).astype(f32) * (TWO_PI / 256)
    x2 = x * x
    s = x * (1.0 + x2 * (-1.0 / 6 + x2 * (1.0 / 120 + x2 * (-1.0 / 5040 + x2 * (1.0 / 362880)))))
    c = 1.0 + x2 * (-0.5 + x2 * (1.0 / 24 + x2 * (-1.0 / 720 + x2 * (1.0 / 40320))))
    odd = (quarter & 1) == 1
    cosine = jnp.where(odd, s, c)
    sine = jnp.where(odd, c, s)
    cosine = jnp.where(((quarter + 1) & 2) == 2, -cosine, cosine)
    sine = jnp.where((quarter & 2) == 2, -sine, sine)
    return cosine, sine


def dot(a, b, dims=((1,), (0,))):
    return lax.dot_general(a, b, (dims, ((), ())), preferred_element_type=f32)


def row(values, k):
    return values[k : k + 1, :]


def x_steps(kx):
    return [unit_circle((kx * j) & (NX - 1)) for j in range(1, 4)]


def x_terms(weights, g, steps):
    even = row(weights[0], g)
    odd = 0.0
    for j in range(1, 4):
        w = row(weights[j], g)
        even = even + w * steps[j - 1][0]
        odd = odd + w * steps[j - 1][1]
    return even, odd


def turned(start, terms):
    cosine, sine = start
    even, odd = terms
    return cosine * even - sine * odd, -(sine * even + cosine * odd)


def placed(rel, weights, g):
    out = jnp.zeros(rel.shape, f32)
    for j in range(4):
        out = jnp.where(rel == j, row(weights[j], g), out)
    return out


def y_rows(spots, weights, g):
    block, local, *weights = (
        jnp.broadcast_to(row(v, g), (16, ATOMS)).astype(bf16) for v in (*spots, *weights)
    )
    nothing = jnp.zeros((16, ATOMS), bf16)
    rel = lax.broadcasted_iota(jnp.int32, (16, ATOMS), 0).astype(f32).astype(bf16) - local
    low = high = nothing
    for j in range(4):
        low = jnp.where(rel == j, weights[j], low)
        high = jnp.where(rel == j - 16, weights[j], high)
    own = [block == b for b in range(16)]
    return jnp.concatenate(
        [jnp.where(own[b], low, jnp.where(own[b - 1], high, nothing)) for b in range(16)], axis=0
    )


def y_spots(by):
    return (by >> 4).astype(f32), (by & 15).astype(f32)


def kernel_pack(count_ref, charge_hbm, frac_hbm, base_hbm, out_ref, factor_ref, charge_ref, frac_ref, base_ref, sems):
    moves = ((charge_hbm, charge_ref), (frac_hbm, frac_ref), (base_hbm, base_ref))
    copies = [pltpu.make_async_copy(a, b, sems.at[i]) for i, (a, b) in enumerate(moves)]
    for copy in copies:
        copy.start()
    for copy in copies:
        copy.wait()
    live = lax.broadcasted_iota(jnp.int32, (1, ATOMS), 1) < count_ref[0]
    loaded = jnp.where(live, charge_ref[...], 0.0)
    rows = [loaded, frac_ref[...], base_ref[...].astype(f32)]
    for g in range(GROUPS):
        out_ref[g] = jnp.concatenate(rows + [jnp.full((1, ATOMS), float(g), f32)], axis=0)
    factor_ref[...] = jnp.concatenate([jnp.where(live, 1.0, 0.0), loaded, loaded, loaded], axis=0)


def whole(values):
    return values.astype(jnp.int32)


def own_waves(atoms_ref):
    return whole(atoms_ref[7, 0:1, :]) * KX + lax.broadcasted_iota(jnp.int32, (KX, ATOMS), 0)


def kernel_spread(sent_ref, table_ref, out_ref, y_ref, x_ref, atoms_ref, lead_ref):
    for k in range(8):
        atoms_ref[k] = sent_ref[:, k, :]
    kx = own_waves(atoms_ref)
    steps = x_steps(kx)
    charge = atoms_ref[0]
    wx, wy, wz = (spline(atoms_ref[1 + d]) for d in range(3))
    bx, by, bz = (whole(atoms_ref[4 + d]) for d in range(3))
    ys = y_spots(by)
    z_at = lax.broadcasted_iota(jnp.int32, (16, ATOMS), 0)
    wz = [charge * w for w in wz]
    blank = jnp.zeros((LANES - PLANES * KX, ATOMS), f32)
    for g in range(GROUPS):
        here = pl.ds(g * ATOMS, ATOMS)
        y_ref[:, here] = y_rows(ys, wy, g)
        start = unit_circle((kx * row(bx, g)) & (NX - 1))
        real, imag = turned(start, x_terms(wx, g, steps))
        for k, values in enumerate((real, imag) + start):
            x_ref[k, :, here] = values
        z = placed(z_at - row(bz, g), wz, g)
        lead = [row(z, k) * real for k in range(PLANES)] + [blank]
        lead_ref[0:LANES, here] = jnp.concatenate(lead, axis=0).astype(bf16)
        lead = [row(z, k) * imag for k in range(PLANES)] + [blank]
        lead_ref[LANES : 2 * LANES, here] = jnp.concatenate(lead, axis=0).astype(bf16)
    mesh = dot(y_ref[...], lead_ref[...], ((1,), (1,)))
    mesh = jnp.concatenate([mesh[:, :LANES], mesh[:, LANES:]], axis=0)
    waves = dot(table_ref[...], mesh.astype(bf16))
    rows = 2 * SLABS
    lane = lax.broadcasted_iota(jnp.int32, (rows, LANES), 1)
    turn = [waves[k * rows : (k + 1) * rows] for k in range(KY)]
    turn = turn[:1] + [pltpu.roll(turn[k], LANES - k * (LANES - SPAN), 1) for k in range(1, KY)]
    packed = [jnp.where(lane < LANES - (k + 1) * (LANES - SPAN), turn[k], turn[k + 1]) for k in range(KY - 1)]
    out_ref[...] = jnp.concatenate(packed, axis=1).astype(bf16).reshape(SENT)


def kernel_waves(mesh_ref, green_ref, table_ref, cos_ref, sin_ref, out_ref, part_ref, back_ref):
    mesh = mesh_ref[...].reshape(2 * SLABS, KY * SPAN)
    part_ref[...] = dot(mesh, table_ref[...], ((0,), (0,)))
    blank = jnp.zeros((SPAN - PLANES * KX, 2 * LANES), f32)
    for k in range(KY):
        real = [None] * 4
        imag = [None] * 4
        for z in range(PLANES):
            at = k * SPAN + z * KX
            a = part_ref[at : at + KX, :LANES]
            b = part_ref[at : at + KX, LANES:]
            for m in range(4):
                if z == 0:
                    real[m], imag[m] = a, b
                    continue
                c = cos_ref[z : z + 1, m * LANES : (m + 1) * LANES]
                s = sin_ref[z : z + 1, m * LANES : (m + 1) * LANES]
                real[m] = real[m] + (a * c + b * s)
                imag[m] = imag[m] + (b * c - a * s)
        for m in range(4):
            factor = green_ref[:, k, m * LANES : (m + 1) * LANES] * (1.0 / (NY * NZ))
            real[m] = real[m] * factor
            imag[m] = imag[m] * factor
        rows = []
        for z in range(PLANES):
            a = b = 0.0
            for m in range(4):
                if z == 0:
                    a, b = a + real[m], b + imag[m]
                    continue
                c = cos_ref[z : z + 1, m * LANES : (m + 1) * LANES]
                s = sin_ref[z : z + 1, m * LANES : (m + 1) * LANES]
                a = a + (real[m] * c - imag[m] * s)
                b = b + (imag[m] * c + real[m] * s)
            rows.append(jnp.concatenate([a, b], axis=1))
        back_ref[k * SPAN : (k + 1) * SPAN] = jnp.concatenate(rows + [blank], axis=0).astype(bf16)
    cells = dot(table_ref[...], back_ref[...], ((1,), (1,)))
    out_ref[...] = cells.astype(bf16).reshape(SENT)


def kernel_sample(atoms_ref, mesh_ref, table_ref, y_ref, x_ref, out_ref, slope_ref):
    kx = own_waves(atoms_ref)
    steps = x_steps(kx)
    wz = spline(atoms_ref[3])
    dx, dy, dz = (spline_slopes(atoms_ref[1 + d]) for d in range(3))
    by, bz = (whole(atoms_ref[4 + d]) for d in range(1, 3))
    ys = y_spots(by)
    z_at = lax.broadcasted_iota(jnp.int32, (16, ATOMS), 0)
    waves = mesh_ref[...].reshape(2 * SLABS, KY * SPAN).T
    waves = jnp.concatenate([waves[k * SPAN : (k + 1) * SPAN] for k in range(KY)], axis=1)
    cells = dot(waves, table_ref[...]).astype(bf16)
    used = PLANES * KX
    cells = jnp.concatenate([cells[:used, :NY], cells[:used, NY:]], axis=0)

    def sample_block(g, level, slope):
        x_real, x_imag, *start = (x_ref[k, :, pl.ds(g * ATOMS, ATOMS)] for k in range(4))
        s_real, s_imag = turned(start, x_terms(dx, g, steps))
        z = placed(z_at - row(bz, g), wz, g)
        dzt = placed(z_at - row(bz, g), dz, g)
        plain = [0.0, 0.0]
        along_y = [0.0, 0.0]
        along_z = [0.0, 0.0]
        for part in range(2):
            for k in range(PLANES):
                at = part * used + k * KX
                here = level[at : at + KX]
                there = slope[at : at + KX]
                plain[part] = plain[part] + row(z, k) * here
                along_y[part] = along_y[part] + row(z, k) * there
                along_z[part] = along_z[part] + row(dzt, k) * here
        terms = (
            x_real * plain[0] + x_imag * plain[1],
            s_real * plain[0] + s_imag * plain[1],
            x_real * along_y[0] + x_imag * along_y[1],
            x_real * along_z[0] + x_imag * along_z[1],
        )
        out_ref[g] = jnp.concatenate([jnp.sum(t, axis=0, keepdims=True) for t in terms], axis=0)

    for g in range(GROUPS):
        here = pl.ds(g * ATOMS, ATOMS)
        slope_ref[:, here] = y_rows(ys, dy, g)
        if g % 2 == 0:
            continue
        both = pl.ds((g - 1) * ATOMS, 2 * ATOMS)
        level = dot(cells, y_ref[:, both])
        slope = dot(cells, slope_ref[:, both])
        for h in range(2):
            at = slice(h * ATOMS, (h + 1) * ATOMS)
            sample_block(g - 1 + h, level[:, at], slope[:, at])


def call(kernel, shape, dtype, inputs, scratch=(), flops=0, limit=8):
    return pl.pallas_call(
        kernel,
        out_shape=jax.ShapeDtypeStruct(shape, dtype),
        in_specs=[VMEM] * inputs,
        out_specs=VMEM,
        scratch_shapes=scratch,
        name=kernel.__name__,
        compiler_params=pltpu.CompilerParams(vmem_limit_bytes=limit << 20),
        cost_estimate=pl.CostEstimate(flops=flops, bytes_accessed=1 << 20, transcendentals=0),
    )


def pack(counts, charge, frac, base):
    return pl.pallas_call(
        kernel_pack,
        out_shape=[
            jax.ShapeDtypeStruct((GROUPS, 8, ATOMS), f32),
            jax.ShapeDtypeStruct((4, ATOMS), f32),
        ],
        in_specs=[pl.BlockSpec(memory_space=pltpu.SMEM)] + [pl.BlockSpec(memory_space=pltpu.HBM)] * 3,
        out_specs=[VMEM, VMEM],
        scratch_shapes=[
            pltpu.VMEM((1, ATOMS), f32),
            pltpu.VMEM((3, ATOMS), f32),
            pltpu.VMEM((3, ATOMS), jnp.int32),
            pltpu.SemaphoreType.DMA((3,)),
        ],
        name="kernel_pack",
        compiler_params=pltpu.CompilerParams(vmem_limit_bytes=4 << 20),
        cost_estimate=pl.CostEstimate(flops=1 << 30, bytes_accessed=1 << 20, transcendentals=0),
    )(counts, *(pltpu.with_memory_space_constraint(a, pltpu.HBM) for a in (charge, frac, base)))


def spread(atoms):
    return pl.pallas_call(
        kernel_spread,
        out_shape=[
            jax.ShapeDtypeStruct(SENT, bf16),
            jax.ShapeDtypeStruct((NY, GROUPS * ATOMS), bf16),
            jax.ShapeDtypeStruct((4, KX, GROUPS * ATOMS), f32),
            jax.ShapeDtypeStruct((8, GROUPS, ATOMS), f32),
        ],
        in_specs=[VMEM] * 2,
        out_specs=[VMEM] * 4,
        scratch_shapes=[pltpu.VMEM((2 * LANES, GROUPS * ATOMS), bf16)],
        name="kernel_spread",
        compiler_params=pltpu.CompilerParams(vmem_limit_bytes=8 << 20),
        cost_estimate=pl.CostEstimate(flops=1 << 30, bytes_accessed=1 << 20, transcendentals=0),
    )(atoms, jnp.asarray(y_table()))


def wave_product(mesh, green):
    scratch = [pltpu.VMEM((KY * SPAN, 2 * LANES), f32), pltpu.VMEM((KY * SPAN, 2 * LANES), bf16)]
    run = call(kernel_waves, SENT, bf16, 5, scratch, 1 << 30)
    return run(mesh, green, jnp.asarray(slab_table()), *map(jnp.asarray, plane_table()))


def sample(atoms, mesh, y_weights, x_sums):
    scratch = [pltpu.VMEM((NY, GROUPS * ATOMS), bf16)]
    run = call(kernel_sample, (GROUPS, 4, ATOMS), f32, 5, scratch, 1 << 30)
    return run(atoms, mesh, jnp.asarray(y_table()), y_weights, x_sums)


def total(factors, terms):
    return jnp.sum(terms, axis=0) * factors


def body(charge, base, frac, counts, green):
    charge = charge.reshape(1, ATOMS)
    swap = functools.partial(lax.all_to_all, split_axis=0, concat_axis=0, tiled=True)
    packed, factors = pack(counts, charge, frac, base)
    atoms = swap(packed, "grp")
    mesh, y_weights, x_sums, atoms = spread(atoms)
    mesh = swap(mesh, "pme")
    mesh = swap(wave_product(mesh, green), "pme")
    terms = swap(sample(atoms, mesh, y_weights, x_sums), "grp")
    return total(factors, terms)


def solution(mesh):
    both = ("grp", "pme")
    placed_in = (P(both), P(None, both), P(None, both), P(both), P("grp", "pme", None))
    return jax.shard_map(body, mesh=mesh, in_specs=placed_in, out_specs=P(None, both), check_vma=False)
```
